128 devices in a mesh: view: 8 (over z, core), tile: 16 (over x, y).
Axes of the slice: x: 4, y: 4, z: 4, core: 2. Of those that a mesh axis runs over, the one named last changes fastest.
Arguments:
- sdf_value: float32 [24576, 256], P(('view', 'tile')), may hold values from -1 to 1
- weight: float32 [24576, 256], P(('view', 'tile')), may hold values from 0.25 to 4
- color: float32 [3, 24576, 256], P(None, ('view', 'tile')), may hold values from 0 to 1
- voxel_index: int32 [24576, 256], P(('view', 'tile')), may hold values from 0 to 511
- valid: int32 [24576, 256], P(('view', 'tile')), may hold values 0 or 1
- list_count: int32 [24576], P(('view', 'tile')), may hold values from 1 to 256
- list_key: int32 [24576], P(('view', 'tile')), may hold values from 0 to 8191, as said below
- owner_slot: int32 [8192], replicated, may hold values from 0 to 8191, as said below
Outputs:
- joined_tsdf: float32 [8192, 512], P(('view', 'tile'))
- joined_color: float32 [8192, 3, 512], P(('view', 'tile'))
- block_counts: int32 [8192], replicated
The draws below stay inside these ranges and needn't reach their ends.
Inputs may be any that keep to these rules, and one draw needn't show every extreme that they name: `owner_slot`: each block key has one storage row and each row one key. Of the 192 lists of one device, at most 6 have a storage row owner_slot[list_key] among the 64 rows of any one device; some device receives exactly 6 lists from every device.
All inputs are finite; a program needn't handle non-finite values. No bound on the sum of `valid` on one device may be relied on, other than what follows from the above.
Results may differ from the reference program's by a relative error of at most 0.0037.
Values may be sent and summed in bfloat16 or wider, within the bound.
No kernel may reach another device: no remote copies, remote signals or barrier semaphores. Data moves between devices by JAX's collectives and lax.ppermute only.
A program may use at most 64 MiB of HBM per device.

```python
import math
import jax
import jax.numpy as jnp
from jax import lax

VOX = 512
PTS = 256
LISTS_DEV = 192
BLK_DEV = 64
CAP = 6
LISTS = 24576
NBLK = 8192
DEVICES = 128


def routing(key):
    base = jax.random.fold_in(key, 7)
    slot_of = jax.random.permutation(jax.random.fold_in(base, 1), NBLK).astype(jnp.int32)
    key_of = jnp.zeros((NBLK,), jnp.int32).at[slot_of].set(jnp.arange(NBLK, dtype=jnp.int32))
    hottest = jax.random.randint(jax.random.fold_in(base, 2), (), 0, DEVICES).astype(jnp.int32)

    def one_source(sub):
        picks = jax.random.permutation(jax.random.fold_in(sub, 0), (DEVICES - 1) * CAP)[:LISTS_DEV - CAP].astype(jnp.int32)
        others = picks // CAP
        others = jnp.where(others >= hottest, others + 1, others)
        targets = jnp.concatenate([jnp.full((CAP,), hottest, jnp.int32), others])
        targets = jax.random.permutation(jax.random.fold_in(sub, 1), targets)
        local_rows = jax.random.randint(jax.random.fold_in(sub, 2), (LISTS_DEV,), 0, BLK_DEV).astype(jnp.int32)
        return key_of[targets * BLK_DEV + local_rows]
    random_subkeys = jax.random.split(jax.random.fold_in(base, 3), DEVICES)
    list_keys = jax.vmap(one_source)(random_subkeys).reshape(-1).astype(jnp.int32)
    return (slot_of, list_keys)


def draw_owner_slot(key, part):
    return routing(key)[0]


def draw_list_key(key, part):
    return routing(key)[1]


def place_ends(array, stream_key, least, top_value):
    longest = array.shape.index(max(array.shape))
    spots = []
    for shift in (0, 1):
        where = [jax.random.randint(jax.random.fold_in(stream_key, axis), (), 0, length) for axis, length in enumerate(array.shape)]
        where[longest] = (where[longest] + shift) % array.shape[longest]
        spots.append(tuple(where))
    return array.at[spots[0]].set(least).at[spots[1]].set(top_value)


def levels(key, shape, cuts, low, largest):
    gain = 1.0
    for dim, shards_of in cuts:
        steps = jax.random.uniform(jax.random.fold_in(jax.random.fold_in(key, 6), dim), (shards_of,), jnp.float32, low / len(cuts), largest / len(cuts))
        gain = gain * jnp.repeat(jnp.exp(steps), shape[dim] // shards_of).reshape((-1,) + (1,) * (len(shape) - 1 - dim))
    return gain


def setup_inputs(seed: int = 0) -> dict:
    streams_of = jax.random.split(jax.random.key(seed), 9)
    sdf_value = jnp.clip(jax.random.uniform(streams_of[0], (LISTS, PTS), jnp.float32, -1.0, 1.0) * levels(streams_of[0], (LISTS, PTS), ((0, 128),), -0.4, 0.0), -1.0, 1.0)
    weight = jnp.clip(jnp.exp(math.log(4.0) - 2.7725887 * jax.random.uniform(streams_of[1], (LISTS, PTS), jnp.float32) ** levels(streams_of[1], (LISTS, PTS), ((0, 128),), -0.2, 0.2)), 0.25, 4.0)
    color = jnp.clip(1.0 * jax.random.uniform(streams_of[2], (3, LISTS, PTS), jnp.float32) ** levels(streams_of[2], (3, LISTS, PTS), ((1, 128),), -0.2, 0.2), 0.0, 1.0)
    voxel_index = place_ends(jax.random.randint(streams_of[3], (LISTS, PTS), 0, VOX), jax.random.fold_in(streams_of[3], 1), 0, VOX - 1).astype(jnp.int32)
    valid = place_ends((jax.random.randint(streams_of[4], (LISTS, PTS), 0, 8) < 7).astype(jnp.int32), jax.random.fold_in(streams_of[4], 1), 0, 1)
    list_count = place_ends(jax.random.randint(streams_of[5], (LISTS,), 1, PTS + 1), jax.random.fold_in(streams_of[5], 1), 1, PTS).astype(jnp.int32)
    list_key = draw_list_key(jax.random.fold_in(streams_of[8], 71), 0)
    owner_slot = draw_owner_slot(jax.random.fold_in(streams_of[8], 71), 0)
    return dict(sdf_value=sdf_value, weight=weight, color=color, voxel_index=voxel_index, valid=valid, list_count=list_count, list_key=list_key, owner_slot=owner_slot)


def reference(sdf_value, weight, color, voxel_index, valid, list_count, list_key, owner_slot):
    points = sdf_value.shape[1]
    position = jnp.arange(points, dtype=jnp.int32)
    live_mask = ((position[None, :] < list_count[:, None]) & (valid == 1)).astype(jnp.float32)
    scaled = live_mask * weight
    channels = jnp.stack([live_mask, scaled, scaled * sdf_value, scaled * color[0], scaled * color[1], scaled * color[2]], axis=-1)
    rounded = lax.optimization_barrier(channels.astype(jnp.bfloat16))
    value_entries = rounded.astype(jnp.float32)
    storage = owner_slot[list_key].astype(jnp.int32)
    segment_ids = (storage[:, None] * VOX + voxel_index).astype(jnp.int32)
    voxel_sums = jax.ops.segment_sum(value_entries.reshape(-1, 6), segment_ids.reshape(-1), num_segments=NBLK * VOX)
    voxel_sums = voxel_sums.reshape(NBLK, VOX, 6)
    block_counts = jnp.sum(voxel_sums[:, :, 0], axis=1).astype(jnp.int32)
    divisor = jnp.maximum(voxel_sums[:, :, 1], 1.0)
    joined_tsdf = voxel_sums[:, :, 2] / divisor
    joined_color = jnp.transpose(voxel_sums[:, :, 3:6] / divisor[:, :, None], (0, 2, 1))
    return joined_tsdf, joined_color, block_counts
```

```python
import jax
import jax.numpy as jnp
from jax import lax
from jax.experimental import pallas as pl
from jax.experimental.pallas import tpu as pltpu
from jax.sharding import PartitionSpec as P

AXES = ("view", "tile")
DEVICES = 128
LISTS = 192
PTS = 256
BLOCKS = 64
CAP = 6
VALUES = 6
ROWS = CAP * VALUES * 2
HIGH = 8
LOW = 64
STRIDE = 72
META = 256
STEP = 16
F32 = jnp.float32
BF16 = jnp.bfloat16
I32 = jnp.int32
VMEM = pl.BlockSpec(memory_space=pltpu.VMEM)
NT = (((1,), (1,)), ((), ()))


def iota(shape, dim):
    return lax.broadcasted_iota(I32, shape, dim)


def hot(cond):
    return jnp.where(cond, 1.0, 0.0).astype(BF16)


def dot(a, b):
    return jnp.dot(a, b, preferred_element_type=F32)


def pack_kernel(sdf, weight, color, voxel, valid, count, key, table, send, meta, x, rows):
    key_row = key[...]
    high_hot = hot((key_row >> 7) == iota((64, LISTS), 0))
    low_hot = jnp.where((key_row & 127) == iota((128, LISTS), 0), 1.0, 0.0)
    slots = table[...]
    owner_of = (slots >> 6).astype(F32).T.astype(BF16)
    row_of = (slots & 63).astype(F32).T.astype(BF16)
    owner = jnp.sum(dot(owner_of, high_hot) * low_hot, axis=0, keepdims=True)
    row = jnp.sum(dot(row_of, high_hot) * low_hot, axis=0, keepdims=True)
    owner_hot = jnp.where(owner.astype(I32) == iota((DEVICES, LISTS), 0), 1.0, 0.0)
    before = hot(iota((LISTS, LISTS), 0) < iota((LISTS, LISTS), 1))
    order = jnp.sum(dot(owner_hot.astype(BF16), before) * owner_hot, axis=0, keepdims=True)

    diagonal = iota((LISTS, LISTS), 0) == iota((LISTS, LISTS), 1)
    spread = jnp.where(diagonal, count[...].astype(F32), 0.0).astype(BF16)
    used = dot(spread, jnp.ones((LISTS, PTS), BF16))
    live = (iota((LISTS, PTS), 1).astype(F32) < used) & (valid[...] == 1)
    mask = jnp.where(live, 1.0, 0.0)
    live_count = lax.dot_general(
        jnp.ones((8, PTS), BF16), mask.astype(BF16), NT, preferred_element_type=F32
    )[0:1]
    packed = (owner.astype(I32) * 64 + row.astype(I32)) * 512 + live_count.astype(I32)
    meta[...] = jnp.concatenate([packed, jnp.zeros((1, META - LISTS), I32)], axis=1)

    scaled = mask * weight[...]
    values = [
        (voxel[...] - 256).astype(F32),
        scaled,
        scaled * sdf[...],
        scaled * color[0],
        scaled * color[1],
        scaled * color[2],
    ]
    for v, value in enumerate(values):
        value = value.astype(BF16)
        for half in range(2):
            j = half * VALUES + v
            x[:, j * 128 : (j + 1) * 128] = value[:, half * 128 : (half + 1) * 128]

    for k in range(CAP):
        place = jnp.where(order == k, owner_hot, 0.0).astype(BF16)
        for j in range(0, 2 * VALUES, 2):
            moved = dot(place, x[:, j * 128 : (j + 2) * 128])
            for side in range(2):
                at = k * 2 * VALUES + j + side
                rows[pl.ds(at, DEVICES, stride=STRIDE), :] = moved[
                    :, side * 128 : (side + 1) * 128
                ]

    def convert(i, carry):
        at = pl.multiple_of(i * 144, 144)
        send[pl.ds(at, 144), :] = rows[pl.ds(at, 144), :].astype(BF16)
        return carry

    lax.fori_loop(0, DEVICES // 2, convert, 0)


def count_kernel(gathered, counts, heads):
    me = lax.axis_index("view") * 16 + lax.axis_index("tile")

    def body(s, total):
        line = gathered[pl.ds(s, 1), :]
        storage = line >> 9
        number = (line & 511).astype(F32)
        a = jnp.where((storage >> 7) == iota((64, META), 0), number, 0.0).astype(BF16)
        b = hot((storage & 127) == iota((128, META), 0))
        return total + lax.dot_general(a, b, NT, preferred_element_type=F32)

    counts[...] = lax.fori_loop(
        0, DEVICES, body, jnp.zeros((64, 128), F32), unroll=4
    ).astype(I32)

    turned = gathered[...].T
    mine = ((turned >> 15) == me) & (iota((META, DEVICES), 0) < LISTS)
    row = ((turned >> 9) & 63) + 1
    before = hot(iota((META, META), 1) < iota((META, META), 0))
    order = dot(before, hot(mine)).astype(I32)
    lines = []
    for k in range(CAP):
        at = jnp.sum(jnp.where(mine & (order == k), row, 0), axis=0, keepdims=True)
        lines.append(jnp.where(at == 0, BLOCKS, at - 1))
    lines.append(jnp.full((2, DEVICES), BLOCKS, I32))
    heads[...] = jnp.concatenate(lines, axis=0)


def join_kernel(heads, got, tsdf, color, total, work):
    step = pl.program_id(0)

    @pl.when(step == 0)
    def _():
        total[...] = jnp.zeros_like(total)
        work[...] = jnp.zeros_like(work)

    low_id = iota((LOW, 128), 0).astype(F32)

    def body(i, carry):
        work[0:ROWS, :] = got[i].astype(F32)
        for k in range(CAP):
            a_parts, b_parts = [], []
            for half in range(2):
                at = (2 * k + half) * VALUES
                index = jnp.broadcast_to(work[at : at + 1, :], (8, 128))
                high = jnp.floor(index * (1.0 / LOW))
                low = index - high * LOW
                low_all = jnp.concatenate([low] * (LOW // 8), axis=0)
                b_parts.append(jnp.where(low_all == low_id, 1.0, 0.0))
                group = work[at : at + 8, :]
                a_parts.append(
                    jnp.concatenate(
                        [jnp.where(high == float(h - 4), group, 0.0) for h in range(HIGH)],
                        axis=0,
                    )
                )
            a = jnp.concatenate(a_parts, axis=1).astype(BF16)
            b = jnp.concatenate(b_parts, axis=1).astype(BF16)
            part = lax.dot_general(a, b, NT, preferred_element_type=F32)
            where = pl.ds(pl.multiple_of(heads[k, step * STEP + i] * STRIDE, 8), HIGH * 8)
            total[where, 0:LOW] += part
        return carry

    lax.fori_loop(0, STEP, body, 0)

    @pl.when(step == DEVICES // STEP - 1)
    def _():
        for h in range(HIGH):

            def channel(c):
                return total[pl.ds(h * 8 + c, BLOCKS, stride=STRIDE), :][:, 0:LOW]

            span = slice(h * LOW, (h + 1) * LOW)
            divisor = jnp.maximum(channel(1), 1.0)
            tsdf[:, span] = channel(2) / divisor
            for c in range(3):
                color[c, :, span] = channel(3 + c) / divisor


def on_device(sdf_value, weight, color, voxel_index, valid, list_count, list_key, owner_slot):
    send, meta = pl.pallas_call(
        pack_kernel,
        out_shape=(
            jax.ShapeDtypeStruct((DEVICES * ROWS, 128), BF16),
            jax.ShapeDtypeStruct((1, META), I32),
        ),
        in_specs=[VMEM] * 8,
        out_specs=(VMEM, VMEM),
        scratch_shapes=[
            pltpu.VMEM((LISTS, 2 * VALUES * 128), BF16),
            pltpu.VMEM((DEVICES * STRIDE, 128), F32),
        ],
        name="pack",
    )(
        sdf_value,
        weight,
        color,
        voxel_index,
        valid,
        list_count.reshape(1, LISTS),
        list_key.reshape(1, LISTS),
        owner_slot.reshape(64, 128),
    )
    got = lax.all_to_all(
        send.reshape(DEVICES, ROWS, 128), AXES, split_axis=0, concat_axis=0, tiled=True
    )
    gathered = lax.all_gather(meta, AXES, axis=0, tiled=True)
    counts, heads = pl.pallas_call(
        count_kernel,
        out_shape=(
            jax.ShapeDtypeStruct((64, 128), I32),
            jax.ShapeDtypeStruct((8, DEVICES), I32),
        ),
        in_specs=[VMEM],
        out_specs=(VMEM, VMEM),
        cost_estimate=pl.CostEstimate(flops=400_000_000, bytes_accessed=200_000, transcendentals=0),
        name="count",
    )(gathered)
    tsdf, colors = pl.pallas_call(
        join_kernel,
        grid=(DEVICES // STEP,),
        out_shape=(
            jax.ShapeDtypeStruct((BLOCKS, 512), F32),
            jax.ShapeDtypeStruct((3, BLOCKS, 512), F32),
        ),
        in_specs=[
            pl.BlockSpec(memory_space=pltpu.SMEM),
            pl.BlockSpec((STEP, ROWS, 128), lambda g: (g, 0, 0)),
        ],
        out_specs=(
            pl.BlockSpec((BLOCKS, 512), lambda g: (0, 0)),
            pl.BlockSpec((3, BLOCKS, 512), lambda g: (0, 0, 0)),
        ),
        scratch_shapes=[
            pltpu.VMEM(((BLOCKS + 1) * STRIDE, 128), F32),
            pltpu.VMEM((80, 128), F32),
        ],
        name="join",
    )(heads, got)
    return tsdf, jnp.transpose(colors, (1, 0, 2)), counts.reshape(DEVICES * BLOCKS)


def solution(mesh):
    return jax.shard_map(
        on_device,
        mesh=mesh,
        in_specs=(
            P(AXES, None),
            P(AXES, None),
            P(None, AXES, None),
            P(AXES, None),
            P(AXES, None),
            P(AXES),
            P(AXES),
            P(),
        ),
        out_specs=(P(AXES, None), P(AXES, None, None), P()),
        check_vma=False,
    )
```

```python
import jax
import jax.numpy as jnp
from jax import lax
from jax.experimental import pallas as pl
from jax.experimental.pallas import tpu as pltpu
from jax.sharding import PartitionSpec as P

AXES = ("view", "tile")
DEVICES = 128
LISTS = 192
PTS = 256
BLOCKS = 64
CAP = 6
VALUES = 6
DATA = CAP * VALUES * 2
ROWS = DATA + 8
HIGH = 8
LOW = 64
STRIDE = 72
META = 256
SOURCES = 2
WORK = 80
F32 = jnp.float32
BF16 = jnp.bfloat16
I32 = jnp.int32
VMEM = pl.BlockSpec(memory_space=pltpu.VMEM)
NT = (((1,), (1,)), ((), ()))


def iota(shape, dim):
    return lax.broadcasted_iota(I32, shape, dim)


def hot(cond):
    return jnp.where(cond, 1.0, 0.0).astype(BF16)


def dot(a, b):
    return jnp.dot(a, b, preferred_element_type=F32)


def pack_kernel(sdf, weight, color, voxel, valid, count, key, table, send, x, rows):
    key_row = key[...]
    high_hot = hot((key_row >> 7) == iota((64, LISTS), 0))
    low_hot = jnp.where((key_row & 127) == iota((128, LISTS), 0), 1.0, 0.0)
    slots = table[...]
    owner_of = (slots >> 6).astype(F32).T.astype(BF16)
    row_of = (slots & 63).astype(F32).T.astype(BF16)
    owner = jnp.sum(dot(owner_of, high_hot) * low_hot, axis=0, keepdims=True)
    row = jnp.sum(dot(row_of, high_hot) * low_hot, axis=0, keepdims=True)
    owner_hot = jnp.where(owner.astype(I32) == iota((DEVICES, LISTS), 0), 1.0, 0.0)
    before = hot(iota((LISTS, LISTS), 0) < iota((LISTS, LISTS), 1))
    order = jnp.sum(dot(owner_hot.astype(BF16), before) * owner_hot, axis=0, keepdims=True)

    diagonal = iota((LISTS, LISTS), 0) == iota((LISTS, LISTS), 1)
    spread = jnp.where(diagonal, count[...].astype(F32), 0.0).astype(BF16)
    used = dot(spread, jnp.ones((LISTS, PTS), BF16))
    live = (iota((LISTS, PTS), 1).astype(F32) < used) & (valid[...] == 1)
    mask = jnp.where(live, 1.0, 0.0)
    live_count = lax.dot_general(
        jnp.ones((8, PTS), BF16), mask.astype(BF16), NT, preferred_element_type=F32
    )[0:1]
    empty = jnp.zeros((1, META - LISTS), F32)
    lines = []
    for line in (
        jnp.concatenate([owner, empty - 1.0], axis=1),
        jnp.concatenate([row, empty], axis=1),
        jnp.concatenate([live_count, empty], axis=1),
    ):
        lines += [line[:, 0:128], line[:, 128:256]]
    head = jnp.concatenate(lines + [jnp.zeros((2, 128), F32)], axis=0)

    def spread_head(i, carry):
        rows[pl.ds(pl.multiple_of(i * ROWS + DATA, 8), 8), :] = head
        return carry

    lax.fori_loop(0, DEVICES, spread_head, 0, unroll=8)

    scaled = mask * weight[...]
    values = [
        (voxel[...] - 256).astype(F32),
        scaled,
        scaled * sdf[...],
        scaled * color[0],
        scaled * color[1],
        scaled * color[2],
    ]
    for v, value in enumerate(values):
        value = value.astype(BF16)
        for half in range(2):
            j = half * VALUES + v
            x[:, j * 128 : (j + 1) * 128] = value[:, half * 128 : (half + 1) * 128]

    for k in range(CAP):
        place = jnp.where(order == k, owner_hot, 0.0).astype(BF16)
        for j in range(0, 2 * VALUES, 2):
            moved = dot(place, x[:, j * 128 : (j + 2) * 128])
            for side in range(2):
                at = k * 2 * VALUES + j + side
                rows[pl.ds(at, DEVICES, stride=ROWS), :] = moved[
                    :, side * 128 : (side + 1) * 128
                ]

    def convert(i, carry):
        at = pl.multiple_of(i * ROWS, ROWS)
        send[pl.ds(at, ROWS), :] = rows[pl.ds(at, ROWS), :].astype(BF16)
        return carry

    lax.fori_loop(0, DEVICES, convert, 0, unroll=4)


def join_kernel(got, tsdf, color, counts, total, work, info, heads, heads_smem, sem):
    me = lax.axis_index("view") * 16 + lax.axis_index("tile")

    def unpack_head(i, carry):
        info[pl.ds(pl.multiple_of(i * 8, 8), 8), :] = got[i, DATA:ROWS, :].astype(F32)
        return carry

    lax.fori_loop(0, DEVICES, unpack_head, 0, unroll=8)

    def plane(p):
        return jnp.concatenate(
            [info[pl.ds(2 * p + half, DEVICES, stride=8), :] for half in range(2)], axis=1
        )

    mine = jnp.where(plane(0) == me.astype(F32), 1.0, 0.0)
    row = plane(1) + 1.0
    before = hot(iota((META, META), 0) < iota((META, META), 1))
    order = dot(mine.astype(BF16), before)
    found = jnp.zeros((8, DEVICES), F32)
    for k in range(CAP):
        picked = jnp.where((order == k) & (mine > 0.0), row, 0.0).astype(BF16)
        select = hot(iota((8, META), 0) == k)
        found += lax.dot_general(select, picked, NT, preferred_element_type=F32)
    found = found.astype(I32)
    heads[...] = jnp.where(found == 0, BLOCKS, found - 1) * STRIDE
    copy = pltpu.make_async_copy(heads, heads_smem, sem)
    copy.start()

    total[...] = jnp.zeros_like(total)
    work[...] = jnp.zeros_like(work)

    def tally(s, sums):
        line = info[pl.ds(pl.multiple_of(s * 8, 8), 8), :]

        def value(p):
            return jnp.concatenate([line[2 * p : 2 * p + 1], line[2 * p + 1 : 2 * p + 2]], axis=1)

        owner = value(0).astype(I32)
        low = (owner & 1) * BLOCKS + value(1).astype(I32)
        a = jnp.where((owner >> 1) == iota((64, META), 0), value(2), 0.0).astype(BF16)
        b = hot(low == iota((128, META), 0))
        return sums + lax.dot_general(a, b, NT, preferred_element_type=F32)

    sums = lax.fori_loop(0, DEVICES, tally, jnp.zeros((64, 128), F32), unroll=4)
    counts[...] = sums.astype(I32)
    copy.wait()

    low_id = iota((LOW, 128), 0).astype(F32)

    def body(i, carry):
        for src in range(SOURCES):
            base = src * WORK
            work[base : base + DATA, :] = got[i * SOURCES + src, 0:DATA, :].astype(F32)
        parts = []
        for src in range(SOURCES):
            for k in range(CAP):
                a_parts, b_parts = [], []
                for half in range(2):
                    at = src * WORK + (2 * k + half) * VALUES
                    index = jnp.broadcast_to(work[at : at + 1, :], (8, 128))
                    high = jnp.floor(index * (1.0 / LOW))
                    low = index - high * LOW
                    low_all = jnp.concatenate([low] * (LOW // 8), axis=0)
                    b_parts.append(jnp.where(low_all == low_id, 1.0, 0.0))
                    group = work[at : at + 8, :]
                    a_parts.append(
                        jnp.concatenate(
                            [jnp.where(high == float(h - 4), group, 0.0) for h in range(HIGH)],
                            axis=0,
                        )
                    )
                a = jnp.concatenate(a_parts, axis=1).astype(BF16)
                b = jnp.concatenate(b_parts, axis=1).astype(BF16)
                part = lax.dot_general(a, b, NT, preferred_element_type=F32)
                at = pl.multiple_of(heads_smem[k, i * SOURCES + src], 8)
                total[pl.ds(at, HIGH * 8), 0:LOW] += part
        return carry

    lax.fori_loop(0, DEVICES // SOURCES, body, 0)

    for h in range(HIGH):

        def channel(c):
            return total[pl.ds(h * 8 + c, BLOCKS, stride=STRIDE), :][:, 0:LOW]

        span = slice(h * LOW, (h + 1) * LOW)
        divisor = jnp.maximum(channel(1), 1.0)
        tsdf[:, span] = channel(2) / divisor
        for c in range(3):
            color[c, :, span] = channel(3 + c) / divisor


def on_device(sdf_value, weight, color, voxel_index, valid, list_count, list_key, owner_slot):
    send = pl.pallas_call(
        pack_kernel,
        out_shape=jax.ShapeDtypeStruct((DEVICES * ROWS, 128), BF16),
        in_specs=[VMEM] * 8,
        out_specs=VMEM,
        scratch_shapes=[
            pltpu.VMEM((LISTS, 2 * VALUES * 128), BF16),
            pltpu.VMEM((DEVICES * ROWS, 128), F32),
        ],
        compiler_params=pltpu.CompilerParams(vmem_limit_bytes=20 * 2**20),
        name="pack",
    )(
        *(
            pltpu.with_memory_space_constraint(given, pltpu.HBM)
            for given in (
                sdf_value,
                weight,
                color,
                voxel_index,
                valid,
                list_count.reshape(1, LISTS),
                list_key.reshape(1, LISTS),
                owner_slot.reshape(64, 128),
            )
        )
    )
    got = lax.all_to_all(
        send.reshape(DEVICES, ROWS, 128), AXES, split_axis=0, concat_axis=0, tiled=True
    )
    got = pltpu.with_memory_space_constraint(got, pltpu.VMEM)
    tsdf, colors, counts = pl.pallas_call(
        join_kernel,
        out_shape=(
            jax.ShapeDtypeStruct((BLOCKS, 512), F32),
            jax.ShapeDtypeStruct((3, BLOCKS, 512), F32),
            jax.ShapeDtypeStruct((64, 128), I32),
        ),
        in_specs=[VMEM],
        out_specs=(VMEM, VMEM, VMEM),
        scratch_shapes=[
            pltpu.VMEM(((BLOCKS + 1) * STRIDE, 128), F32),
            pltpu.VMEM((SOURCES * WORK, 128), F32),
            pltpu.VMEM((DEVICES * 8, 128), F32),
            pltpu.VMEM((8, DEVICES), I32),
            pltpu.SMEM((8, DEVICES), I32),
            pltpu.SemaphoreType.DMA,
        ],
        compiler_params=pltpu.CompilerParams(vmem_limit_bytes=20 * 2**20),
        name="join",
    )(got)
    return tsdf, jnp.transpose(colors, (1, 0, 2)), counts.reshape(DEVICES * BLOCKS)


def solution(mesh):
    return jax.shard_map(
        on_device,
        mesh=mesh,
        in_specs=(
            P(AXES, None),
            P(AXES, None),
            P(None, AXES, None),
            P(AXES, None),
            P(AXES, None),
            P(AXES),
            P(AXES),
            P(),
        ),
        out_specs=(P(AXES, None), P(AXES, None, None), P()),
        check_vma=False,
    )
```

```python
import jax
import jax.numpy as jnp
from jax import lax
from jax.experimental import pallas as pl
from jax.experimental.pallas import tpu as pltpu
from jax.sharding import PartitionSpec as P

AXES = ("view", "tile")
DEVICES = 128
LISTS = 192
PTS = 256
BLOCKS = 64
CAP = 6
VALUES = 6
DATA = CAP * VALUES * 2
ROWS = DATA + 8
HIGH = 8
LOW = 64
STRIDE = 72
META = 256
SOURCES = 16
TALLY = DEVICES * LISTS // 128
GROUP = 32
WORK = 80
F32 = jnp.float32
BF16 = jnp.bfloat16
I32 = jnp.int32
VMEM = pl.BlockSpec(memory_space=pltpu.VMEM)
NT = (((1,), (1,)), ((), ()))


def iota(shape, dim):
    return lax.broadcasted_iota(I32, shape, dim)


def hot(cond):
    return jnp.where(cond, 1.0, 0.0).astype(BF16)


def dot(a, b):
    return jnp.dot(a, b, preferred_element_type=F32)


def pack_kernel(sdf, weight, color, voxel, valid, count, key, table, send, x, rows):
    key_row = key[...]
    high_hot = hot((key_row >> 7) == iota((64, LISTS), 0))
    low_hot = jnp.where((key_row & 127) == iota((128, LISTS), 0), 1.0, 0.0)
    slots = table[...]
    owner_of = (slots >> 6).astype(F32).T.astype(BF16)
    row_of = (slots & 63).astype(F32).T.astype(BF16)
    owner = jnp.sum(dot(owner_of, high_hot) * low_hot, axis=0, keepdims=True)
    row = jnp.sum(dot(row_of, high_hot) * low_hot, axis=0, keepdims=True)
    owner_hot = jnp.where(owner.astype(I32) == iota((DEVICES, LISTS), 0), 1.0, 0.0)
    before = hot(iota((LISTS, LISTS), 0) < iota((LISTS, LISTS), 1))
    order = jnp.sum(dot(owner_hot.astype(BF16), before) * owner_hot, axis=0, keepdims=True)

    diagonal = iota((LISTS, LISTS), 0) == iota((LISTS, LISTS), 1)
    spread = jnp.where(diagonal, count[...].astype(F32), 0.0).astype(BF16)
    used = dot(spread, jnp.ones((LISTS, PTS), BF16))
    live = (iota((LISTS, PTS), 1).astype(F32) < used) & (valid[...] == 1)
    mask = jnp.where(live, 1.0, 0.0)
    live_count = lax.dot_general(
        jnp.ones((8, PTS), BF16), mask.astype(BF16), NT, preferred_element_type=F32
    )[0:1]
    storage = owner * BLOCKS + row
    high = jnp.floor(storage * (1.0 / 128))
    odd = (lax.axis_index("tile") & 1) == 1
    lines = []
    for line, fill in ((high, -1.0), (storage - high * 128, 0.0), (live_count, 0.0)):
        blank = jnp.full((1, 64), fill, F32)
        rest = line[:, 128:LISTS]
        lines += [
            line[:, 0:128],
            jnp.where(
                odd,
                jnp.concatenate([blank, rest], axis=1),
                jnp.concatenate([rest, blank], axis=1),
            ),
        ]
    head = jnp.concatenate(lines + [jnp.zeros((2, 128), F32)], axis=0)

    def spread_head(i, carry):
        rows[pl.ds(pl.multiple_of(i * ROWS + DATA, 8), 8), :] = head
        return carry

    lax.fori_loop(0, DEVICES, spread_head, 0, unroll=8)

    scaled = mask * weight[...]
    values = [
        (voxel[...] - 256).astype(F32),
        scaled,
        scaled * sdf[...],
        scaled * color[0],
        scaled * color[1],
        scaled * color[2],
    ]
    for v, value in enumerate(values):
        value = value.astype(BF16)
        for half in range(2):
            j = half * VALUES + v
            x[:, j * 128 : (j + 1) * 128] = value[:, half * 128 : (half + 1) * 128]

    for k in range(CAP):
        place = jnp.where(order == k, owner_hot, 0.0).astype(BF16)
        for j in range(0, 2 * VALUES, 2):
            moved = dot(place, x[:, j * 128 : (j + 2) * 128])
            for side in range(2):
                at = k * 2 * VALUES + j + side
                rows[pl.ds(at, DEVICES, stride=ROWS), :] = moved[
                    :, side * 128 : (side + 1) * 128
                ]

    def convert(i, carry):
        at = pl.multiple_of(i * ROWS, ROWS)
        send[pl.ds(at, ROWS), :] = rows[pl.ds(at, ROWS), :].astype(BF16)
        return carry

    lax.fori_loop(0, DEVICES, convert, 0, unroll=4)


def twice(rows8):
    return jnp.concatenate([rows8, rows8], axis=0).astype(BF16)


def ids(count):
    return [(iota((16, 128), 0) + 16 * j).astype(F32).astype(BF16) for j in range(count)]


def join_kernel(got, tsdf, color, counts, total, work, info, lines, heads, heads_smem, sem):
    me = lax.axis_index("view") * 16 + lax.axis_index("tile")
    one, zero = jnp.ones((), BF16), jnp.zeros((), BF16)

    def unpack_head(i, carry):
        info[pl.ds(pl.multiple_of(i * 8, 8), 8), :] = got[i, DATA:ROWS, :].astype(F32)
        return carry

    lax.fori_loop(0, DEVICES, unpack_head, 0, unroll=16)

    def plane(p):
        return jnp.concatenate(
            [info[pl.ds(2 * p + half, DEVICES, stride=8), :] for half in range(2)], axis=1
        )

    row = plane(0) * 128.0 + plane(1) - (me * BLOCKS).astype(F32)
    mine = (row >= 0.0) & (row < float(BLOCKS))
    before = hot(iota((META, META), 0) < iota((META, META), 1))
    order = dot(hot(mine), before)
    found = jnp.zeros((8, DEVICES), F32)
    for k in range(CAP):
        picked = jnp.where((order == k) & mine, row + 1.0, 0.0).astype(BF16)
        select = hot(iota((8, META), 0) == k)
        found += lax.dot_general(select, picked, NT, preferred_element_type=F32)
    found = found.astype(I32)
    heads[...] = jnp.where(found == 0, BLOCKS, found - 1) * STRIDE
    copy = pltpu.make_async_copy(heads, heads_smem, sem)
    copy.start()

    total[...] = jnp.zeros_like(total)
    work[...] = jnp.zeros_like(work)

    left = iota((DEVICES // 2, 128), 1) < 64
    for p in range(3):
        lines[p, 0:DEVICES, :] = info[pl.ds(2 * p, DEVICES, stride=8), :]
        lines[p, DEVICES:TALLY, :] = jnp.where(
            left,
            info[pl.ds(2 * p + 1, DEVICES // 2, stride=16), :],
            info[pl.ds(2 * p + 9, DEVICES // 2, stride=16), :],
        )
    tally_ids = ids(8)

    def tally(g, sums):
        a_parts, b_parts = [], []
        for t in range(GROUP):
            high, low, number = [
                twice(jnp.broadcast_to(lines[p, pl.ds(g * GROUP + t, 1), :], (8, 128)))
                for p in range(3)
            ]
            a_parts.append(
                jnp.concatenate([jnp.where(high == tally_ids[j], number, zero) for j in range(4)], 0)
            )
            b_parts.append(
                jnp.concatenate([jnp.where(low == tally_ids[j], one, zero) for j in range(8)], 0)
            )
        a = jnp.concatenate(a_parts, axis=1)
        b = jnp.concatenate(b_parts, axis=1)
        return sums + lax.dot_general(a, b, NT, preferred_element_type=F32)

    sums = lax.fori_loop(0, TALLY // GROUP, tally, jnp.zeros((64, 128), F32))
    counts[...] = sums.astype(I32)
    copy.wait()

    low_id = iota((LOW, 128), 0).astype(F32).astype(BF16)
    high_id = [
        ((iota((16, 128), 0) >> 3) + (2 * j - 4)).astype(F32).astype(BF16) for j in range(HIGH // 2)
    ]

    def body(i, carry):
        for src in range(SOURCES):
            base = src * WORK
            work[base : base + DATA, :] = got[i * SOURCES + src, 0:DATA, :].astype(F32)
        for src in range(SOURCES):
            for k in range(CAP):
                a_parts, b_parts = [], []
                for half in range(2):
                    at = src * WORK + (2 * k + half) * VALUES
                    index = jnp.broadcast_to(work[at : at + 1, :], (8, 128))
                    high = jnp.floor(index * (1.0 / LOW))
                    low = twice(index - high * LOW)
                    high = twice(high)
                    low_all = jnp.concatenate([low] * (LOW // 16), axis=0)
                    b_parts.append(jnp.where(low_all == low_id, one, zero))
                    group = twice(work[at : at + 8, :])
                    a_parts.append(
                        jnp.concatenate(
                            [jnp.where(high == high_id[j], group, zero) for j in range(HIGH // 2)],
                            axis=0,
                        )
                    )
                a = jnp.concatenate(a_parts, axis=1)
                b = jnp.concatenate(b_parts, axis=1)
                part = lax.dot_general(a, b, NT, preferred_element_type=F32)
                at = pl.multiple_of(heads_smem[k, i * SOURCES + src], 8)
                total[pl.ds(at, HIGH * 8), 0:LOW] += part
        return carry

    lax.fori_loop(0, DEVICES // SOURCES, body, 0)

    for h in range(HIGH):

        def channel(c):
            return total[pl.ds(h * 8 + c, BLOCKS, stride=STRIDE), :][:, 0:LOW]

        span = slice(h * LOW, (h + 1) * LOW)
        divisor = jnp.maximum(channel(1), 1.0)
        tsdf[:, span] = channel(2) / divisor
        for c in range(3):
            color[c, :, span] = channel(3 + c) / divisor


def pack(sdf_value, weight, color, voxel_index, valid, list_count, list_key, owner_slot):
    return pl.pallas_call(
        pack_kernel,
        out_shape=jax.ShapeDtypeStruct((DEVICES * ROWS, 128), BF16),
        in_specs=[VMEM] * 8,
        out_specs=VMEM,
        scratch_shapes=[
            pltpu.VMEM((LISTS, 2 * VALUES * 128), BF16),
            pltpu.VMEM((DEVICES * ROWS, 128), F32),
        ],
        compiler_params=pltpu.CompilerParams(vmem_limit_bytes=20 * 2**20),
        name="pack",
    )(
        *(
            pltpu.with_memory_space_constraint(given, pltpu.HBM)
            for given in (
                sdf_value,
                weight,
                color,
                voxel_index,
                valid,
                list_count.reshape(1, LISTS),
                list_key.reshape(1, LISTS),
                owner_slot.reshape(64, 128),
            )
        )
    )


def join(got):
    return pl.pallas_call(
        join_kernel,
        out_shape=(
            jax.ShapeDtypeStruct((BLOCKS, 512), F32),
            jax.ShapeDtypeStruct((3, BLOCKS, 512), F32),
            jax.ShapeDtypeStruct((64, 128), I32),
        ),
        in_specs=[VMEM],
        out_specs=(VMEM, VMEM, VMEM),
        scratch_shapes=[
            pltpu.VMEM(((BLOCKS + 1) * STRIDE, 128), F32),
            pltpu.VMEM((SOURCES * WORK, 128), F32),
            pltpu.VMEM((DEVICES * 8, 128), F32),
            pltpu.VMEM((3, TALLY, 128), F32),
            pltpu.VMEM((8, DEVICES), I32),
            pltpu.SMEM((8, DEVICES), I32),
            pltpu.SemaphoreType.DMA,
        ],
        compiler_params=pltpu.CompilerParams(vmem_limit_bytes=20 * 2**20),
        name="join",
    )(pltpu.with_memory_space_constraint(got, pltpu.VMEM))


def on_device(*given):
    got = lax.all_to_all(
        pack(*given).reshape(DEVICES, ROWS, 128), AXES, split_axis=0, concat_axis=0, tiled=True
    )
    tsdf, colors, counts = join(got)
    return tsdf, jnp.transpose(colors, (1, 0, 2)), counts.reshape(DEVICES * BLOCKS)


def solution(mesh):
    return jax.shard_map(
        on_device,
        mesh=mesh,
        in_specs=(
            P(AXES, None),
            P(AXES, None),
            P(None, AXES, None),
            P(AXES, None),
            P(AXES, None),
            P(AXES),
            P(AXES),
            P(),
        ),
        out_specs=(P(AXES, None), P(AXES, None, None), P()),
        check_vma=False,
    )
```

```python
import jax
import jax.numpy as jnp
from jax import lax
from jax.experimental import pallas as pl
from jax.experimental.pallas import tpu as pltpu
from jax.sharding import PartitionSpec as P

AXES = ("view", "tile")
DEVICES = 128
LISTS = 192
PTS = 256
BLOCKS = 64
CAP = 6
VALUES = 6
DATA = CAP * VALUES * 2
ROWS = DATA + 8
HIGH = 8
LOW = 64
STRIDE = 72
SPREAD = 84
META = 256
SOURCES = 32
TALLY = DEVICES * LISTS // 128
GROUP = 32
WORK = 80
F32 = jnp.float32
BF16 = jnp.bfloat16
I32 = jnp.int32
VMEM = pl.BlockSpec(memory_space=pltpu.VMEM)
NT = (((1,), (1,)), ((), ()))


def iota(shape, dim):
    return lax.broadcasted_iota(I32, shape, dim)


def hot(cond):
    return jnp.where(cond, 1.0, 0.0).astype(BF16)


def dot(a, b):
    return jnp.dot(a, b, preferred_element_type=F32)


def pack_kernel(*refs):
    given, send, x, rows, place = refs[:8], refs[8], refs[9], refs[10], refs[11]
    held, sems = refs[12:20], refs[20]
    copies = [
        pltpu.make_async_copy(src, dst, sems.at[i]) for i, (src, dst) in enumerate(zip(given, held))
    ]
    for copy in copies:
        copy.start()
    key, table, count, valid, voxel, weight, sdf, color = held

    copies[0].wait()
    copies[1].wait()
    key_row = key[...]
    high_hot = hot((key_row >> 7) == iota((64, LISTS), 0))
    low_hot = jnp.where((key_row & 127) == iota((128, LISTS), 0), 1.0, 0.0)
    slots = table[...]
    owner_of = (slots >> 6).astype(F32).T.astype(BF16)
    row_of = (slots & 63).astype(F32).T.astype(BF16)
    owner = jnp.sum(dot(owner_of, high_hot) * low_hot, axis=0, keepdims=True)
    row = jnp.sum(dot(row_of, high_hot) * low_hot, axis=0, keepdims=True)
    owner_hot = jnp.where(owner.astype(I32) == iota((DEVICES, LISTS), 0), 1.0, 0.0)
    before = hot(iota((LISTS, LISTS), 0) < iota((LISTS, LISTS), 1))
    order = jnp.sum(dot(owner_hot.astype(BF16), before) * owner_hot, axis=0, keepdims=True)
    for k in range(CAP):
        place[k * DEVICES : (k + 1) * DEVICES, :] = jnp.where(order == k, owner_hot, 0.0).astype(
            BF16
        )

    copies[2].wait()
    copies[3].wait()
    diagonal = iota((LISTS, LISTS), 0) == iota((LISTS, LISTS), 1)
    spread = jnp.where(diagonal, count[...].astype(F32), 0.0).astype(BF16)
    used = dot(spread, jnp.ones((LISTS, PTS), BF16))
    live = (iota((LISTS, PTS), 1).astype(F32) < used) & (valid[...] == 1)
    mask = jnp.where(live, 1.0, 0.0)
    live_count = lax.dot_general(
        jnp.ones((8, PTS), BF16), mask.astype(BF16), NT, preferred_element_type=F32
    )[0:1]
    storage = owner * BLOCKS + row
    high = jnp.floor(storage * (1.0 / 128))
    odd = (lax.axis_index("tile") & 1) == 1
    lines = []
    for line, fill in ((high, -1.0), (storage - high * 128, 0.0), (live_count, 0.0)):
        blank = jnp.full((1, 64), fill, F32)
        rest = line[:, 128:LISTS]
        lines += [
            line[:, 0:128],
            jnp.where(
                odd,
                jnp.concatenate([blank, rest], axis=1),
                jnp.concatenate([rest, blank], axis=1),
            ),
        ]
    head = jnp.concatenate(lines + [jnp.zeros((2, 128), F32)], axis=0)

    def spread_head(i, carry):
        rows[pl.ds(i * SPREAD + DATA, 8), :] = head
        return carry

    lax.fori_loop(0, DEVICES, spread_head, 0, unroll=8)

    for copy in copies[4:]:
        copy.wait()
    scaled = mask * weight[...]
    values = [
        (voxel[...] - 256).astype(F32),
        scaled,
        scaled * sdf[...],
        scaled * color[0],
        scaled * color[1],
        scaled * color[2],
    ]
    for v, value in enumerate(values):
        value = value.astype(BF16)
        for half in range(2):
            j = half * VALUES + v
            x[:, j * 128 : (j + 1) * 128] = value[:, half * 128 : (half + 1) * 128]

    for j in range(0, 2 * VALUES, 2):
        for k in range(CAP):
            moved = dot(place[k * DEVICES : (k + 1) * DEVICES, :], x[:, j * 128 : (j + 2) * 128])
            for side in range(2):
                at = k * 2 * VALUES + j + side
                rows[pl.ds(at, DEVICES, stride=SPREAD), :] = moved[:, side * 128 : (side + 1) * 128]

    def convert(i, carry):
        at = pl.multiple_of(i * ROWS, ROWS)
        send[pl.ds(at, ROWS), :] = rows[pl.ds(i * SPREAD, ROWS), :].astype(BF16)
        return carry

    lax.fori_loop(0, DEVICES, convert, 0, unroll=8)


def twice(rows8):
    return jnp.concatenate([rows8, rows8], axis=0).astype(BF16)


def ids(count):
    return [(iota((16, 128), 0) + 16 * j).astype(F32).astype(BF16) for j in range(count)]


def join_kernel(got, tsdf, color, counts, total, work, info, lines, heads, heads_smem, sem):
    me = lax.axis_index("view") * 16 + lax.axis_index("tile")
    one, zero = jnp.ones((), BF16), jnp.zeros((), BF16)

    def unpack_head(i, carry):
        info[pl.ds(pl.multiple_of(i * 8, 8), 8), :] = got[i, DATA:ROWS, :].astype(F32)
        return carry

    lax.fori_loop(0, DEVICES, unpack_head, 0, unroll=16)

    def plane(p):
        return jnp.concatenate(
            [info[pl.ds(2 * p + half, DEVICES, stride=8), :] for half in range(2)], axis=1
        )

    row = plane(0) * 128.0 + plane(1) - (me * BLOCKS).astype(F32)
    mine = (row >= 0.0) & (row < float(BLOCKS))
    before = hot(iota((META, META), 0) < iota((META, META), 1))
    order = dot(hot(mine), before)
    found = jnp.zeros((8, DEVICES), F32)
    for k in range(CAP):
        picked = jnp.where((order == k) & mine, row + 1.0, 0.0).astype(BF16)
        select = hot(iota((8, META), 0) == k)
        found += lax.dot_general(select, picked, NT, preferred_element_type=F32)
    found = found.astype(I32)
    heads[...] = jnp.where(found == 0, BLOCKS, found - 1) * STRIDE
    copy = pltpu.make_async_copy(heads, heads_smem, sem)
    copy.start()

    total[...] = jnp.zeros_like(total)
    work[...] = jnp.zeros_like(work)

    left = iota((DEVICES // 2, 128), 1) < 64
    for p in range(3):
        lines[p, 0:DEVICES, :] = info[pl.ds(2 * p, DEVICES, stride=8), :]
        lines[p, DEVICES:TALLY, :] = jnp.where(
            left,
            info[pl.ds(2 * p + 1, DEVICES // 2, stride=16), :],
            info[pl.ds(2 * p + 9, DEVICES // 2, stride=16), :],
        )
    tally_ids = ids(8)

    def tally(g, sums):
        a_parts, b_parts = [], []
        for t in range(GROUP):
            high, low, number = [
                twice(jnp.broadcast_to(lines[p, pl.ds(g * GROUP + t, 1), :], (8, 128)))
                for p in range(3)
            ]
            a_parts.append(
                jnp.concatenate([jnp.where(high == tally_ids[j], number, zero) for j in range(4)], 0)
            )
            b_parts.append(
                jnp.concatenate([jnp.where(low == tally_ids[j], one, zero) for j in range(8)], 0)
            )
        a = jnp.concatenate(a_parts, axis=1)
        b = jnp.concatenate(b_parts, axis=1)
        return sums + lax.dot_general(a, b, NT, preferred_element_type=F32)

    sums = lax.fori_loop(0, TALLY // GROUP, tally, jnp.zeros((64, 128), F32))
    counts[...] = sums.astype(I32)
    copy.wait()

    low_id = iota((LOW, 128), 0).astype(F32).astype(BF16)
    high_id = [
        ((iota((16, 128), 0) >> 3) + (2 * j - 4)).astype(F32).astype(BF16) for j in range(HIGH // 2)
    ]

    def body(i, carry):
        for src in range(SOURCES):
            base = src * WORK
            work[base : base + DATA, :] = got[i * SOURCES + src, 0:DATA, :].astype(F32)
        for src in range(SOURCES):
            for k in range(CAP):
                a_parts, b_parts = [], []
                for half in range(2):
                    at = src * WORK + (2 * k + half) * VALUES
                    index = jnp.broadcast_to(work[at : at + 1, :], (8, 128))
                    high = jnp.floor(index * (1.0 / LOW))
                    low = twice(index - high * LOW)
                    high = twice(high)
                    low_all = jnp.concatenate([low] * (LOW // 16), axis=0)
                    b_parts.append(jnp.where(low_all == low_id, one, zero))
                    group = twice(work[at : at + 8, :])
                    a_parts.append(
                        jnp.concatenate(
                            [jnp.where(high == high_id[j], group, zero) for j in range(HIGH // 2)],
                            axis=0,
                        )
                    )
                a = jnp.concatenate(a_parts, axis=1)
                b = jnp.concatenate(b_parts, axis=1)
                part = lax.dot_general(a, b, NT, preferred_element_type=F32)
                at = pl.multiple_of(heads_smem[k, i * SOURCES + src], 8)
                total[pl.ds(at, HIGH * 8), 0:LOW] += part
        return carry

    lax.fori_loop(0, DEVICES // SOURCES, body, 0)

    for h in range(HIGH):

        def channel(c):
            return total[pl.ds(h * 8 + c, BLOCKS, stride=STRIDE), :][:, 0:LOW]

        span = slice(h * LOW, (h + 1) * LOW)
        divisor = jnp.maximum(channel(1), 1.0)
        tsdf[:, span] = channel(2) / divisor
        for c in range(3):
            color[c, :, span] = channel(3 + c) / divisor


def pack(sdf_value, weight, color, voxel_index, valid, list_count, list_key, owner_slot):
    given = (
        list_key.reshape(1, LISTS),
        owner_slot.reshape(64, 128),
        list_count.reshape(1, LISTS),
        valid,
        voxel_index,
        weight,
        sdf_value,
        color,
    )
    return pl.pallas_call(
        pack_kernel,
        out_shape=jax.ShapeDtypeStruct((DEVICES * ROWS, 128), BF16),
        in_specs=[pl.BlockSpec(memory_space=pl.ANY)] * 8,
        out_specs=VMEM,
        scratch_shapes=[
            pltpu.VMEM((LISTS, 2 * VALUES * 128), BF16),
            pltpu.VMEM((DEVICES * SPREAD, 128), F32),
            pltpu.VMEM((CAP * DEVICES, LISTS), BF16),
            *(pltpu.VMEM(array.shape, array.dtype) for array in given),
            pltpu.SemaphoreType.DMA((8,)),
        ],
        compiler_params=pltpu.CompilerParams(vmem_limit_bytes=20 * 2**20),
        name="pack",
    )(*(pltpu.with_memory_space_constraint(array, pltpu.HBM) for array in given))


def join(got):
    return pl.pallas_call(
        join_kernel,
        out_shape=(
            jax.ShapeDtypeStruct((BLOCKS, 512), F32),
            jax.ShapeDtypeStruct((3, BLOCKS, 512), F32),
            jax.ShapeDtypeStruct((64, 128), I32),
        ),
        in_specs=[VMEM],
        out_specs=(VMEM, VMEM, VMEM),
        scratch_shapes=[
            pltpu.VMEM(((BLOCKS + 1) * STRIDE, 128), F32),
            pltpu.VMEM((SOURCES * WORK, 128), F32),
            pltpu.VMEM((DEVICES * 8, 128), F32),
            pltpu.VMEM((3, TALLY, 128), F32),
            pltpu.VMEM((8, DEVICES), I32),
            pltpu.SMEM((8, DEVICES), I32),
            pltpu.SemaphoreType.DMA,
        ],
        compiler_params=pltpu.CompilerParams(vmem_limit_bytes=20 * 2**20),
        name="join",
    )(pltpu.with_memory_space_constraint(got, pltpu.VMEM))


def on_device(*given):
    got = lax.all_to_all(
        pack(*given).reshape(DEVICES, ROWS, 128), AXES, split_axis=0, concat_axis=0, tiled=True
    )
    tsdf, colors, counts = join(got)
    return tsdf, jnp.transpose(colors, (1, 0, 2)), counts.reshape(DEVICES * BLOCKS)


def solution(mesh):
    return jax.shard_map(
        on_device,
        mesh=mesh,
        in_specs=(
            P(AXES, None),
            P(AXES, None),
            P(None, AXES, None),
            P(AXES, None),
            P(AXES, None),
            P(AXES),
            P(AXES),
            P(),
        ),
        out_specs=(P(AXES, None), P(AXES, None, None), P()),
        check_vma=False,
    )
```

```python
import jax
import jax.numpy as jnp
from jax import lax
from jax.experimental import pallas as pl
from jax.experimental.pallas import tpu as pltpu
from jax.sharding import PartitionSpec as P

AXES = ("view", "tile")
DEVICES = 128
LISTS = 192
PTS = 256
BLOCKS = 64
CAP = 6
VALUES = 6
DATA = CAP * VALUES * 2
ROWS = DATA + 4
PAIR = 2 * ROWS
GAP = 20
HIGH = 8
LOW = 64
STRIDE = 72
META = 256
SOURCES = 32
TALLY = DEVICES * LISTS // 128
GROUP = 32
F32 = jnp.float32
BF16 = jnp.bfloat16
I32 = jnp.int32
VMEM = pl.BlockSpec(memory_space=pltpu.VMEM)
NT = (((1,), (1,)), ((), ()))


def iota(shape, dim):
    return lax.broadcasted_iota(I32, shape, dim)


def hot(cond):
    return jnp.where(cond, 1.0, 0.0).astype(BF16)


def dot(a, b):
    return jnp.dot(a, b, preferred_element_type=F32)


def pack_kernel(*refs):
    given, send, x, rows, place = refs[:8], refs[8], refs[9], refs[10], refs[11]
    held, sems = refs[12:20], refs[20]
    copies = [
        pltpu.make_async_copy(src, dst, sems.at[i]) for i, (src, dst) in enumerate(zip(given, held))
    ]
    for copy in copies:
        copy.start()
    key, table, count, valid, voxel, weight, sdf, color = held

    copies[0].wait()
    copies[1].wait()
    key_row = key[...]
    high_hot = hot((key_row >> 7) == iota((64, LISTS), 0))
    low_hot = jnp.where((key_row & 127) == iota((128, LISTS), 0), 1.0, 0.0)
    slots = table[...]
    owner_of = (slots >> 6).astype(F32).T.astype(BF16)
    row_of = (slots & 63).astype(F32).T.astype(BF16)
    owner = jnp.sum(dot(owner_of, high_hot) * low_hot, axis=0, keepdims=True)
    row = jnp.sum(dot(row_of, high_hot) * low_hot, axis=0, keepdims=True)
    owner_hot = jnp.where(owner.astype(I32) == iota((DEVICES, LISTS), 0), 1.0, 0.0)
    before = hot(iota((LISTS, LISTS), 0) < iota((LISTS, LISTS), 1))
    order = jnp.sum(dot(owner_hot.astype(BF16), before) * owner_hot, axis=0, keepdims=True)
    for k in range(CAP):
        place[k * DEVICES : (k + 1) * DEVICES, :] = jnp.where(order == k, owner_hot, 0.0).astype(
            BF16
        )

    copies[2].wait()
    copies[3].wait()
    diagonal = iota((LISTS, LISTS), 0) == iota((LISTS, LISTS), 1)
    spread = jnp.where(diagonal, count[...].astype(F32), 0.0).astype(BF16)
    used = dot(spread, jnp.ones((LISTS, PTS), BF16))
    live = (iota((LISTS, PTS), 1).astype(F32) < used) & (valid[...] == 1)
    mask = jnp.where(live, 1.0, 0.0)
    live_count = lax.dot_general(
        jnp.ones((8, PTS), BF16), mask.astype(BF16), NT, preferred_element_type=F32
    )[0:1]
    storage = owner * BLOCKS + row
    high = jnp.floor(storage * (1.0 / 128))
    code = storage - high * 128.0 + 128.0
    high_bits = high.astype(I32)
    for bit in range(6):
        code = jnp.where((high_bits >> bit) & 1 == 1, code * 2.0 ** (1 << bit), code)
    odd = (lax.axis_index("tile") & 1) == 1
    blank = jnp.zeros((1, 64), F32)
    lines = []
    for line in (code, live_count):
        rest = line[:, 128:LISTS]
        lines += [
            line[:, 0:128],
            jnp.where(
                odd,
                jnp.concatenate([blank, rest], axis=1),
                jnp.concatenate([rest, blank], axis=1),
            ),
        ]
    head = jnp.concatenate(lines, axis=0)

    def spread_head(i, carry):
        rows[pl.ds(i * ROWS + DATA, 4), :] = head
        return carry

    lax.fori_loop(0, DEVICES, spread_head, 0, unroll=8)

    for copy in copies[4:]:
        copy.wait()
    scaled = mask * weight[...]
    values = [
        (voxel[...] - 256).astype(F32),
        scaled,
        scaled * sdf[...],
        scaled * color[0],
        scaled * color[1],
        scaled * color[2],
    ]
    for v, value in enumerate(values):
        value = value.astype(BF16)
        for half in range(2):
            j = half * VALUES + v
            x[:, j * 128 : (j + 1) * 128] = value[:, half * 128 : (half + 1) * 128]

    for j in range(0, 2 * VALUES, 2):
        for k in range(CAP):
            moved = dot(place[k * DEVICES : (k + 1) * DEVICES, :], x[:, j * 128 : (j + 2) * 128])
            for side in range(2):
                at = k * 2 * VALUES + j + side
                rows[pl.ds(at, DEVICES, stride=ROWS), :] = moved[:, side * 128 : (side + 1) * 128]

    def convert(i, carry):
        at = pl.multiple_of(i * PAIR, PAIR)
        send[pl.ds(at, PAIR), :] = rows[pl.ds(at, PAIR), :].astype(BF16)
        return carry

    lax.fori_loop(0, DEVICES // 2, convert, 0, unroll=4)


def twice(rows8):
    return jnp.concatenate([rows8, rows8], axis=0).astype(BF16)


def ids(count):
    return [(iota((16, 128), 0) + 16 * j).astype(F32).astype(BF16) for j in range(count)]


def join_kernel(got, tsdf, color, counts, total, work, info, lines, heads, heads_smem, sem):
    me = lax.axis_index("view") * 16 + lax.axis_index("tile")
    one, zero = jnp.ones((), BF16), jnp.zeros((), BF16)

    def unpack_head(i, carry):
        for side in range(2):
            at = pl.multiple_of(i * PAIR + DATA * (side + 1), 8)
            info[pl.ds(i * GAP + 8 * side, 8), :] = got[pl.ds(at, 8), :].astype(F32)
        return carry

    lax.fori_loop(0, DEVICES // 2, unpack_head, 0, unroll=16)

    def line(p):
        return jnp.concatenate(
            [info[pl.ds(p + 12 * side, DEVICES // 2, stride=GAP), :] for side in range(2)], axis=0
        )

    def decoded(code):
        high = jnp.zeros_like(code)
        for bit in range(5, -1, -1):
            step = float(1 << bit)
            over = code >= 128.0 * 2.0**step
            code = jnp.where(over, code * 2.0**-step, code)
            high = jnp.where(over, high + step, high)
        return high, code - 128.0

    full = (*decoded(line(0)), line(2))
    rest = (*decoded(line(1)), line(3))
    row = jnp.concatenate([full[0] * 128.0 + full[1], rest[0] * 128.0 + rest[1]], axis=1)
    row = row - (me * BLOCKS).astype(F32)
    mine = (row >= 0.0) & (row < float(BLOCKS))
    before = hot(iota((META, META), 0) < iota((META, META), 1))
    order = dot(hot(mine), before)
    found = jnp.zeros((8, DEVICES), F32)
    for k in range(CAP):
        picked = jnp.where((order == k) & mine, row + 1.0, 0.0).astype(BF16)
        select = hot(iota((8, META), 0) == k)
        found += lax.dot_general(select, picked, NT, preferred_element_type=F32)
    found = found.astype(I32)
    heads[...] = jnp.where(found == 0, BLOCKS, found - 1) * STRIDE
    copy = pltpu.make_async_copy(heads, heads_smem, sem)
    copy.start()

    total[...] = jnp.zeros_like(total)

    left = iota((DEVICES // 2, 128), 1) < 64
    for p in range(3):
        lines[p, 0:DEVICES, :] = full[p]
        lines[p, DEVICES:TALLY, :] = jnp.where(
            left, rest[p][0 : DEVICES // 2], rest[p][DEVICES // 2 : DEVICES]
        )
    tally_ids = ids(8)

    def tally(g, sums):
        a_parts, b_parts = [], []
        for t in range(GROUP):
            high, low, number = [
                twice(jnp.broadcast_to(lines[p, pl.ds(g * GROUP + t, 1), :], (8, 128)))
                for p in range(3)
            ]
            a_parts.append(
                jnp.concatenate([jnp.where(high == tally_ids[j], number, zero) for j in range(4)], 0)
            )
            b_parts.append(
                jnp.concatenate([jnp.where(low == tally_ids[j], one, zero) for j in range(8)], 0)
            )
        a = jnp.concatenate(a_parts, axis=1)
        b = jnp.concatenate(b_parts, axis=1)
        return sums + lax.dot_general(a, b, NT, preferred_element_type=F32)

    sums = lax.fori_loop(0, TALLY // GROUP, tally, jnp.zeros((64, 128), F32))
    counts[...] = sums.astype(I32)
    copy.wait()

    low_id = iota((LOW, 128), 0).astype(F32).astype(BF16)
    high_id = [
        ((iota((16, 128), 0) >> 3) + (2 * j - 4)).astype(F32).astype(BF16) for j in range(HIGH // 2)
    ]

    def body(i, carry):
        for pair in range(SOURCES // 2):
            at = pl.multiple_of((i * (SOURCES // 2) + pair) * PAIR, 8)
            work[pair * PAIR : (pair + 1) * PAIR, :] = got[pl.ds(at, PAIR), :].astype(F32)
        for src in range(SOURCES):
            for k in range(CAP):
                a_parts, b_parts = [], []
                for half in range(2):
                    at = src * ROWS + (2 * k + half) * VALUES
                    index = jnp.broadcast_to(work[at : at + 1, :], (8, 128))
                    high = jnp.floor(index * (1.0 / LOW))
                    low = twice(index - high * LOW)
                    high = twice(high)
                    low_all = jnp.concatenate([low] * (LOW // 16), axis=0)
                    b_parts.append(jnp.where(low_all == low_id, one, zero))
                    group = twice(work[at : at + 8, :])
                    a_parts.append(
                        jnp.concatenate(
                            [jnp.where(high == high_id[j], group, zero) for j in range(HIGH // 2)],
                            axis=0,
                        )
                    )
                a = jnp.concatenate(a_parts, axis=1)
                b = jnp.concatenate(b_parts, axis=1)
                part = lax.dot_general(a, b, NT, preferred_element_type=F32)
                at = pl.multiple_of(heads_smem[k, i * (SOURCES // 2) + src // 2 + src % 2 * (DEVICES // 2)], 8)
                total[pl.ds(at, HIGH * 8), 0:LOW] += part
        return carry

    lax.fori_loop(0, DEVICES // SOURCES, body, 0)

    for h in range(HIGH):

        def channel(c):
            return total[pl.ds(h * 8 + c, BLOCKS, stride=STRIDE), :][:, 0:LOW]

        span = slice(h * LOW, (h + 1) * LOW)
        divisor = jnp.maximum(channel(1), 1.0)
        tsdf[:, span] = channel(2) / divisor
        for c in range(3):
            color[c, :, span] = channel(3 + c) / divisor


def pack(sdf_value, weight, color, voxel_index, valid, list_count, list_key, owner_slot):
    given = (
        list_key.reshape(1, LISTS),
        owner_slot.reshape(64, 128),
        list_count.reshape(1, LISTS),
        valid,
        voxel_index,
        weight,
        sdf_value,
        color,
    )
    return pl.pallas_call(
        pack_kernel,
        out_shape=jax.ShapeDtypeStruct((DEVICES * ROWS, 128), BF16),
        in_specs=[pl.BlockSpec(memory_space=pl.ANY)] * 8,
        out_specs=VMEM,
        scratch_shapes=[
            pltpu.VMEM((LISTS, 2 * VALUES * 128), BF16),
            pltpu.VMEM((DEVICES * ROWS, 128), F32),
            pltpu.VMEM((CAP * DEVICES, LISTS), BF16),
            *(pltpu.VMEM(array.shape, array.dtype) for array in given),
            pltpu.SemaphoreType.DMA((8,)),
        ],
        compiler_params=pltpu.CompilerParams(vmem_limit_bytes=20 * 2**20),
        name="pack",
    )(*(pltpu.with_memory_space_constraint(array, pltpu.HBM) for array in given))


def join(got):
    return pl.pallas_call(
        join_kernel,
        out_shape=(
            jax.ShapeDtypeStruct((BLOCKS, 512), F32),
            jax.ShapeDtypeStruct((3, BLOCKS, 512), F32),
            jax.ShapeDtypeStruct((64, 128), I32),
        ),
        in_specs=[VMEM],
        out_specs=(VMEM, VMEM, VMEM),
        scratch_shapes=[
            pltpu.VMEM(((BLOCKS + 1) * STRIDE, 128), F32),
            pltpu.VMEM((SOURCES * ROWS, 128), F32),
            pltpu.VMEM((DEVICES // 2 * GAP, 128), F32),
            pltpu.VMEM((3, TALLY, 128), F32),
            pltpu.VMEM((8, DEVICES), I32),
            pltpu.SMEM((8, DEVICES), I32),
            pltpu.SemaphoreType.DMA,
        ],
        compiler_params=pltpu.CompilerParams(vmem_limit_bytes=20 * 2**20),
        name="join",
    )(pltpu.with_memory_space_constraint(got, pltpu.VMEM))


def on_device(*given):
    send = pack(*given).reshape(DEVICES, ROWS // 2, 2, 128)
    got = lax.all_to_all(send, AXES, split_axis=0, concat_axis=0, tiled=True)
    tsdf, colors, counts = join(got.reshape(DEVICES * ROWS, 128))
    return tsdf, jnp.transpose(colors, (1, 0, 2)), counts.reshape(DEVICES * BLOCKS)


def solution(mesh):
    return jax.shard_map(
        on_device,
        mesh=mesh,
        in_specs=(
            P(AXES, None),
            P(AXES, None),
            P(None, AXES, None),
            P(AXES, None),
            P(AXES, None),
            P(AXES),
            P(AXES),
            P(),
        ),
        out_specs=(P(AXES, None), P(AXES, None, None), P()),
        check_vma=False,
    )
```

```python
import jax
import jax.numpy as jnp
from jax import lax
from jax.experimental import pallas as pl
from jax.experimental.pallas import tpu as pltpu
from jax.sharding import PartitionSpec as P

AXES = ("view", "tile")
DEVICES = 128
LISTS = 192
PTS = 256
BLOCKS = 64
CAP = 6
VALUES = 6
DATA = CAP * VALUES * 2
ROWS = DATA + 4
PAIR = 2 * ROWS
GAP = 20
HIGH = 8
LOW = 64
STRIDE = 40
META = 256
SOURCES = 32
TALLY = DEVICES * LISTS // 128
GROUP = 32
F32 = jnp.float32
BF16 = jnp.bfloat16
I32 = jnp.int32
F8 = jnp.float8_e4m3fn
VMEM = pl.BlockSpec(memory_space=pltpu.VMEM)
NT = (((1,), (1,)), ((), ()))


def iota(shape, dim):
    return lax.broadcasted_iota(I32, shape, dim)


def hot(cond):
    return jnp.where(cond, 1.0, 0.0).astype(BF16)


def dot(a, b):
    return jnp.dot(a, b, preferred_element_type=F32)


def pack_kernel(*refs):
    given, send, x, rows, place = refs[:8], refs[8], refs[9], refs[10], refs[11]
    held, sems = refs[12:20], refs[20]
    copies = [
        pltpu.make_async_copy(src, dst, sems.at[i]) for i, (src, dst) in enumerate(zip(given, held))
    ]
    for copy in copies:
        copy.start()
    key, table, count, valid, voxel, weight, sdf, color = held

    copies[0].wait()
    copies[1].wait()
    key_row = key[...]
    high_hot = hot((key_row >> 7) == iota((64, LISTS), 0))
    low_hot = jnp.where((key_row & 127) == iota((128, LISTS), 0), 1.0, 0.0)
    slots = table[...]
    owner_of = (slots >> 6).astype(F32).T.astype(BF16)
    row_of = (slots & 63).astype(F32).T.astype(BF16)
    owner = jnp.sum(dot(owner_of, high_hot) * low_hot, axis=0, keepdims=True)
    row = jnp.sum(dot(row_of, high_hot) * low_hot, axis=0, keepdims=True)
    owner_hot = jnp.where(owner.astype(I32) == iota((DEVICES, LISTS), 0), 1.0, 0.0)
    before = hot(iota((LISTS, LISTS), 0) < iota((LISTS, LISTS), 1))
    order = jnp.sum(dot(owner_hot.astype(BF16), before) * owner_hot, axis=0, keepdims=True)
    for k in range(CAP):
        place[k * DEVICES : (k + 1) * DEVICES, :] = jnp.where(order == k, owner_hot, 0.0).astype(
            BF16
        )

    copies[2].wait()
    copies[3].wait()
    diagonal = iota((LISTS, LISTS), 0) == iota((LISTS, LISTS), 1)
    spread = jnp.where(diagonal, count[...].astype(F32), 0.0).astype(BF16)
    used = dot(spread, jnp.ones((LISTS, PTS), BF16))
    live = (iota((LISTS, PTS), 1).astype(F32) < used) & (valid[...] == 1)
    mask = jnp.where(live, 1.0, 0.0)
    live_count = lax.dot_general(
        jnp.ones((8, PTS), BF16), mask.astype(BF16), NT, preferred_element_type=F32
    )[0:1]
    storage = owner * BLOCKS + row
    high = jnp.floor(storage * (1.0 / 128))
    code = storage - high * 128.0 + 128.0
    high_bits = high.astype(I32)
    for bit in range(6):
        code = jnp.where((high_bits >> bit) & 1 == 1, code * 2.0 ** (1 << bit), code)
    odd = (lax.axis_index("tile") & 1) == 1
    blank = jnp.zeros((1, 64), F32)
    lines = []
    for line in (code, live_count):
        rest = line[:, 128:LISTS]
        lines += [
            line[:, 0:128],
            jnp.where(
                odd,
                jnp.concatenate([blank, rest], axis=1),
                jnp.concatenate([rest, blank], axis=1),
            ),
        ]
    head = jnp.concatenate(lines, axis=0)

    def spread_head(i, carry):
        rows[pl.ds(i * ROWS + DATA, 4), :] = head
        return carry

    lax.fori_loop(0, DEVICES, spread_head, 0, unroll=8)

    for copy in copies[4:]:
        copy.wait()
    scaled = mask * weight[...]
    values = [
        (voxel[...] - 256).astype(F32),
        scaled,
        scaled * sdf[...],
        scaled * color[0],
        scaled * color[1],
        scaled * color[2],
    ]
    for v, value in enumerate(values):
        value = value.astype(BF16)
        for half in range(2):
            j = half * VALUES + v
            x[:, j * 128 : (j + 1) * 128] = value[:, half * 128 : (half + 1) * 128]

    for j in range(0, 2 * VALUES, 2):
        for k in range(CAP):
            moved = dot(place[k * DEVICES : (k + 1) * DEVICES, :], x[:, j * 128 : (j + 2) * 128])
            for side in range(2):
                at = k * 2 * VALUES + j + side
                rows[pl.ds(at, DEVICES, stride=ROWS), :] = moved[:, side * 128 : (side + 1) * 128]

    def convert(i, carry):
        at = pl.multiple_of(i * PAIR, PAIR)
        send[pl.ds(at, PAIR), :] = rows[pl.ds(at, PAIR), :].astype(BF16)
        return carry

    lax.fori_loop(0, DEVICES // 2, convert, 0, unroll=4)


def twice(rows8):
    return jnp.concatenate([rows8, rows8], axis=0).astype(BF16)


def ids(count):
    return [(iota((16, 128), 0) + 16 * j).astype(F32).astype(BF16) for j in range(count)]


def join_kernel(got, tsdf, color, counts, total, work, info, lines, heads, heads_smem, sem):
    me = lax.axis_index("view") * 16 + lax.axis_index("tile")
    one, zero = jnp.ones((), BF16), jnp.zeros((), BF16)

    def unpack_head(i, carry):
        for side in range(2):
            at = pl.multiple_of(i * PAIR + DATA * (side + 1), 8)
            info[pl.ds(i * GAP + 8 * side, 8), :] = got[pl.ds(at, 8), :].astype(F32)
        return carry

    lax.fori_loop(0, DEVICES // 2, unpack_head, 0, unroll=16)

    def line(p):
        return jnp.concatenate(
            [info[pl.ds(p + 12 * side, DEVICES // 2, stride=GAP), :] for side in range(2)], axis=0
        )

    def decoded(code):
        high = jnp.zeros_like(code)
        for bit in range(5, -1, -1):
            step = float(1 << bit)
            over = code >= 128.0 * 2.0**step
            code = jnp.where(over, code * 2.0**-step, code)
            high = jnp.where(over, high + step, high)
        return high, code - 128.0

    full = (*decoded(line(0)), line(2))
    rest = (*decoded(line(1)), line(3))
    row = jnp.concatenate([full[0] * 128.0 + full[1], rest[0] * 128.0 + rest[1]], axis=1)
    row = row - (me * BLOCKS).astype(F32)
    mine = (row >= 0.0) & (row < float(BLOCKS))
    before = hot(iota((META, META), 0) < iota((META, META), 1))
    order = dot(hot(mine), before)
    found = jnp.zeros((8, DEVICES), F32)
    for k in range(CAP):
        picked = jnp.where((order == k) & mine, row + 1.0, 0.0).astype(BF16)
        select = hot(iota((8, META), 0) == k)
        found += lax.dot_general(select, picked, NT, preferred_element_type=F32)
    found = found.astype(I32)
    heads[...] = jnp.where(found == 0, BLOCKS, found - 1) * STRIDE
    copy = pltpu.make_async_copy(heads, heads_smem, sem)
    copy.start()

    total[...] = jnp.zeros_like(total)

    left = iota((DEVICES // 2, 128), 1) < 64
    for p in range(3):
        lines[p, 0:DEVICES, :] = full[p]
        lines[p, DEVICES:TALLY, :] = jnp.where(
            left, rest[p][0 : DEVICES // 2], rest[p][DEVICES // 2 : DEVICES]
        )
    tally_ids = ids(8)

    def tally(g, sums):
        a_parts, b_parts = [], []
        for t in range(GROUP):
            high, low, number = [
                twice(jnp.broadcast_to(lines[p, pl.ds(g * GROUP + t, 1), :], (8, 128)))
                for p in range(3)
            ]
            a_parts.append(
                jnp.concatenate([jnp.where(high == tally_ids[j], number, zero) for j in range(4)], 0)
            )
            b_parts.append(
                jnp.concatenate([jnp.where(low == tally_ids[j], one, zero) for j in range(8)], 0)
            )
        a = jnp.concatenate(a_parts, axis=1)
        b = jnp.concatenate(b_parts, axis=1).astype(F8)
        return sums + lax.dot_general(a, b, NT, preferred_element_type=F32)

    sums = lax.fori_loop(0, TALLY // GROUP, tally, jnp.zeros((64, 128), F32))
    counts[...] = sums.astype(I32)
    copy.wait()

    low_id = iota((LOW, 128), 0).astype(F32).astype(BF16)
    high_id = ((iota((16, 128), 0) & 7) - 4).astype(F32).astype(BF16)

    def body(i, carry):
        for pair in range(SOURCES // 2):
            at = pl.multiple_of((i * (SOURCES // 2) + pair) * PAIR, 8)
            work[pair * PAIR : (pair + 1) * PAIR, :] = got[pl.ds(at, PAIR), :].astype(F32)
        for src in range(SOURCES):
            for k in range(CAP):
                a_parts, b_parts = [], []
                for half in range(2):
                    at = src * ROWS + (2 * k + half) * VALUES
                    index = twice(jnp.broadcast_to(work[at : at + 1, :], (8, 128)))
                    high = jnp.floor(index * (1.0 / LOW))
                    low = index - high * LOW
                    low_all = jnp.concatenate([low] * (LOW // 16), axis=0)
                    b_parts.append(jnp.where(low_all == low_id, one, zero))
                    here = high == high_id
                    wide = [
                        jnp.broadcast_to(work[at + c : at + c + 1, :], (8, 128))
                        for c in range(1, VALUES)
                    ]
                    wide.append(wide[-1])
                    a_parts.append(
                        jnp.concatenate(
                            [
                                jnp.where(
                                    here,
                                    jnp.concatenate(wide[c : c + 2], axis=0).astype(BF16),
                                    zero,
                                )
                                for c in range(0, VALUES, 2)
                            ],
                            axis=0,
                        )
                    )
                a = jnp.concatenate(a_parts, axis=1)
                b = jnp.concatenate(b_parts, axis=1).astype(F8)
                part = lax.dot_general(a, b, NT, preferred_element_type=F32)
                at = pl.multiple_of(heads_smem[k, i * (SOURCES // 2) + src // 2 + src % 2 * (DEVICES // 2)], 8)
                total[pl.ds(at, STRIDE), 0:LOW] += part[0:STRIDE]
        return carry

    lax.fori_loop(0, DEVICES // SOURCES, body, 0)

    for h in range(HIGH):

        def channel(c):
            return total[pl.ds((c - 1) * HIGH + h, BLOCKS, stride=STRIDE), :][:, 0:LOW]

        span = slice(h * LOW, (h + 1) * LOW)
        divisor = jnp.maximum(channel(1), 1.0)
        tsdf[:, span] = channel(2) / divisor
        for c in range(3):
            color[c, :, span] = channel(3 + c) / divisor


def pack(sdf_value, weight, color, voxel_index, valid, list_count, list_key, owner_slot):
    given = (
        list_key.reshape(1, LISTS),
        owner_slot.reshape(64, 128),
        list_count.reshape(1, LISTS),
        valid,
        voxel_index,
        weight,
        sdf_value,
        color,
    )
    return pl.pallas_call(
        pack_kernel,
        out_shape=jax.ShapeDtypeStruct((DEVICES * ROWS, 128), BF16),
        in_specs=[pl.BlockSpec(memory_space=pl.ANY)] * 8,
        out_specs=VMEM,
        scratch_shapes=[
            pltpu.VMEM((LISTS, 2 * VALUES * 128), BF16),
            pltpu.VMEM((DEVICES * ROWS, 128), F32),
            pltpu.VMEM((CAP * DEVICES, LISTS), BF16),
            *(pltpu.VMEM(array.shape, array.dtype) for array in given),
            pltpu.SemaphoreType.DMA((8,)),
        ],
        compiler_params=pltpu.CompilerParams(vmem_limit_bytes=20 * 2**20),
        name="pack",
    )(*(pltpu.with_memory_space_constraint(array, pltpu.HBM) for array in given))


def join(got):
    return pl.pallas_call(
        join_kernel,
        out_shape=(
            jax.ShapeDtypeStruct((BLOCKS, 512), F32),
            jax.ShapeDtypeStruct((3, BLOCKS, 512), F32),
            jax.ShapeDtypeStruct((64, 128), I32),
        ),
        in_specs=[VMEM],
        out_specs=(VMEM, VMEM, VMEM),
        scratch_shapes=[
            pltpu.VMEM(((BLOCKS + 1) * STRIDE, 128), F32),
            pltpu.VMEM((SOURCES * ROWS, 128), F32),
            pltpu.VMEM((DEVICES // 2 * GAP, 128), F32),
            pltpu.VMEM((3, TALLY, 128), F32),
            pltpu.VMEM((8, DEVICES), I32),
            pltpu.SMEM((8, DEVICES), I32),
            pltpu.SemaphoreType.DMA,
        ],
        compiler_params=pltpu.CompilerParams(vmem_limit_bytes=20 * 2**20),
        name="join",
    )(pltpu.with_memory_space_constraint(got, pltpu.VMEM))


def on_device(*given):
    send = pack(*given).reshape(DEVICES, ROWS // 2, 2, 128)
    got = lax.all_to_all(send, AXES, split_axis=0, concat_axis=0, tiled=True)
    tsdf, colors, counts = join(got.reshape(DEVICES * ROWS, 128))
    return tsdf, jnp.transpose(colors, (1, 0, 2)), counts.reshape(DEVICES * BLOCKS)


def solution(mesh):
    return jax.shard_map(
        on_device,
        mesh=mesh,
        in_specs=(
            P(AXES, None),
            P(AXES, None),
            P(None, AXES, None),
            P(AXES, None),
            P(AXES, None),
            P(AXES),
            P(AXES),
            P(),
        ),
        out_specs=(P(AXES, None), P(AXES, None, None), P()),
        check_vma=False,
    )
```

```python
import jax
import jax.numpy as jnp
from jax import lax
from jax.experimental import pallas as pl
from jax.experimental.pallas import tpu as pltpu
from jax.sharding import PartitionSpec as P

AXES = ("view", "tile")
DEVICES = 128
LISTS = 192
PTS = 256
BLOCKS = 64
CAP = 6
VALUES = 6
DATA = CAP * VALUES * 2
ROWS = DATA + 4
PAIR = 2 * ROWS
SIDE = DEVICES // 2
GAP = 20
HIGH = 8
LOW = 64
STRIDE = 40
META = 256
SOURCES = 32
TALLY = DEVICES * LISTS // 128
GROUP = 32
F32 = jnp.float32
BF16 = jnp.bfloat16
I32 = jnp.int32
F8 = jnp.float8_e4m3fn
VMEM = pl.BlockSpec(memory_space=pltpu.VMEM)
NT = (((1,), (1,)), ((), ()))


def iota(shape, dim):
    return lax.broadcasted_iota(I32, shape, dim)


def hot(cond):
    return jnp.where(cond, 1.0, 0.0).astype(BF16)


def dot(a, b):
    return jnp.dot(a, b, preferred_element_type=F32)


def pack_kernel(*refs):
    given, send, x, place, rows = refs[:8], refs[8], refs[9], refs[10], refs[11:13]
    held, sems = refs[13:21], refs[21]
    copies = [
        pltpu.make_async_copy(src, dst, sems.at[i]) for i, (src, dst) in enumerate(zip(given, held))
    ]
    for copy in copies:
        copy.start()
    key, table, count, valid, voxel, weight, sdf, color = held

    copies[0].wait()
    copies[1].wait()
    key_row = key[...]
    high_hot = hot((key_row >> 7) == iota((64, LISTS), 0))
    low_hot = jnp.where((key_row & 127) == iota((128, LISTS), 0), 1.0, 0.0)
    slots = table[...]
    owner_of = (slots >> 6).astype(F32).T.astype(BF16)
    row_of = (slots & 63).astype(F32).T.astype(BF16)
    owner = jnp.sum(dot(owner_of, high_hot) * low_hot, axis=0, keepdims=True)
    row = jnp.sum(dot(row_of, high_hot) * low_hot, axis=0, keepdims=True)
    owner_hot = jnp.where(owner.astype(I32) == iota((DEVICES, LISTS), 0), 1.0, 0.0)
    before = hot(iota((LISTS, LISTS), 0) < iota((LISTS, LISTS), 1))
    order = jnp.sum(dot(owner_hot.astype(BF16), before) * owner_hot, axis=0, keepdims=True)
    for side in range(2):
        for k in range(CAP):
            at = (side * CAP + k) * SIDE
            place[at : at + SIDE, :] = jnp.where(
                order == k, owner_hot[side * SIDE : (side + 1) * SIDE], 0.0
            ).astype(BF16)

    copies[2].wait()
    copies[3].wait()
    diagonal = iota((LISTS, LISTS), 0) == iota((LISTS, LISTS), 1)
    spread = jnp.where(diagonal, count[...].astype(F32), 0.0).astype(BF16)
    used = dot(spread, jnp.ones((LISTS, PTS), BF16))
    live = (iota((LISTS, PTS), 1).astype(F32) < used) & (valid[...] == 1)
    mask = jnp.where(live, 1.0, 0.0)
    live_count = lax.dot_general(
        jnp.ones((8, PTS), BF16), mask.astype(BF16), NT, preferred_element_type=F32
    )[0:1]
    storage = owner * BLOCKS + row
    high = jnp.floor(storage * (1.0 / 128))
    code = storage - high * 128.0 + 128.0
    high_bits = high.astype(I32)
    for bit in range(6):
        code = jnp.where((high_bits >> bit) & 1 == 1, code * 2.0 ** (1 << bit), code)
    odd = (lax.axis_index("tile") & 1) == 1
    blank = jnp.zeros((1, 64), F32)
    lines = []
    for line in (code, live_count):
        rest = line[:, 128:LISTS]
        lines += [
            line[:, 0:128],
            jnp.where(
                odd,
                jnp.concatenate([blank, rest], axis=1),
                jnp.concatenate([rest, blank], axis=1),
            ),
        ]
    head = jnp.concatenate(lines, axis=0)

    for i in range(SIDE):
        for side in range(2):
            rows[side][i * ROWS + DATA : (i + 1) * ROWS, :] = head

    for copy in copies[4:]:
        copy.wait()
    scaled = mask * weight[...]
    values = [
        (voxel[...] - 256).astype(F32),
        scaled,
        scaled * sdf[...],
        scaled * color[0],
        scaled * color[1],
        scaled * color[2],
    ]
    for v, value in enumerate(values):
        value = value.astype(BF16)
        for half in range(2):
            j = half * VALUES + v
            x[:, j * 128 : (j + 1) * 128] = value[:, half * 128 : (half + 1) * 128]

    def move(side, j):
        span = slice(side * CAP * SIDE, (side + 1) * CAP * SIDE)
        moved = dot(place[span, :], x[:, j * 128 : (j + 2) * 128])
        for k in range(CAP):
            for part in range(2):
                at = k * 2 * VALUES + j + part
                rows[side][pl.ds(at, SIDE, stride=ROWS), :] = moved[
                    k * SIDE : (k + 1) * SIDE, part * 128 : (part + 1) * 128
                ]

    def convert(side, pair):
        at = pair * PAIR
        to = side * SIDE * ROWS + at
        send[to : to + PAIR, :] = rows[side][at : at + PAIR, :].astype(BF16)

    for j in range(0, 2 * VALUES, 2):
        move(0, j)
    for j in range(0, 2 * VALUES, 2):
        move(1, j)
        for pair in range(j * SIDE // 24, (j + 2) * SIDE // 24):
            convert(0, pair)
    for pair in range(SIDE // 2):
        convert(1, pair)


def twice(rows8):
    return jnp.concatenate([rows8, rows8], axis=0).astype(BF16)


def ids(count):
    return [(iota((16, 128), 0) + 16 * j).astype(F32).astype(BF16) for j in range(count)]


def join_kernel(
    got, tsdf, color, counts, total, work, info, lines, heads, heads_smem, sem, tsdf_now, color_now,
    counts_now, out_sems
):
    me = lax.axis_index("view") * 16 + lax.axis_index("tile")
    one, zero = jnp.ones((), BF16), jnp.zeros((), BF16)

    def unpack_head(i, carry):
        for side in range(2):
            at = pl.multiple_of(i * PAIR + DATA * (side + 1), 8)
            info[pl.ds(i * GAP + 8 * side, 8), :] = got[pl.ds(at, 8), :].astype(F32)
        return carry

    lax.fori_loop(0, DEVICES // 2, unpack_head, 0, unroll=16)

    def line(p):
        return jnp.concatenate(
            [info[pl.ds(p + 12 * side, DEVICES // 2, stride=GAP), :] for side in range(2)], axis=0
        )

    def decoded(code):
        high = jnp.zeros_like(code)
        for bit in range(5, -1, -1):
            step = float(1 << bit)
            over = code >= 128.0 * 2.0**step
            code = jnp.where(over, code * 2.0**-step, code)
            high = jnp.where(over, high + step, high)
        return high, code - 128.0

    full = (*decoded(line(0)), line(2))
    rest = (*decoded(line(1)), line(3))
    row = jnp.concatenate([full[0] * 128.0 + full[1], rest[0] * 128.0 + rest[1]], axis=1)
    row = row - (me * BLOCKS).astype(F32)
    mine = (row >= 0.0) & (row < float(BLOCKS))
    before = hot(iota((META, META), 0) < iota((META, META), 1))
    order = dot(hot(mine), before)
    found = jnp.zeros((8, DEVICES), F32)
    for k in range(CAP):
        picked = jnp.where((order == k) & mine, row + 1.0, 0.0).astype(BF16)
        select = hot(iota((8, META), 0) == k)
        found += lax.dot_general(select, picked, NT, preferred_element_type=F32)
    found = found.astype(I32)
    heads[...] = jnp.where(found == 0, BLOCKS, found - 1) * STRIDE
    copy = pltpu.make_async_copy(heads, heads_smem, sem)
    copy.start()

    total[...] = jnp.zeros_like(total)

    left = iota((DEVICES // 2, 128), 1) < 64
    for p in range(3):
        lines[p, 0:DEVICES, :] = full[p]
        lines[p, DEVICES:TALLY, :] = jnp.where(
            left, rest[p][0 : DEVICES // 2], rest[p][DEVICES // 2 : DEVICES]
        )
    tally_ids = ids(8)

    def tally(g, sums):
        a_parts, b_parts = [], []
        for t in range(GROUP):
            high, low, number = [
                twice(jnp.broadcast_to(lines[p, pl.ds(g * GROUP + t, 1), :], (8, 128)))
                for p in range(3)
            ]
            a_parts.append(
                jnp.concatenate([jnp.where(high == tally_ids[j], number, zero) for j in range(4)], 0)
            )
            b_parts.append(
                jnp.concatenate([jnp.where(low == tally_ids[j], one, zero) for j in range(8)], 0)
            )
        a = jnp.concatenate(a_parts, axis=1)
        b = jnp.concatenate(b_parts, axis=1).astype(F8)
        return sums + lax.dot_general(a, b, NT, preferred_element_type=F32)

    sums = lax.fori_loop(0, TALLY // GROUP, tally, jnp.zeros((64, 128), F32))
    counts_now[...] = sums.astype(I32)
    copies = [pltpu.make_async_copy(counts_now, counts, out_sems.at[0])]
    copies[0].start()
    copy.wait()

    low_id = iota((LOW, 128), 0).astype(F32).astype(BF16)
    high_id = ((iota((16, 128), 0) & 7) - 4).astype(F32).astype(BF16)

    def body(i, carry):
        for pair in range(SOURCES // 2):
            at = pl.multiple_of((i * (SOURCES // 2) + pair) * PAIR, 8)
            work[pair * PAIR : (pair + 1) * PAIR, :] = got[pl.ds(at, PAIR), :].astype(F32)
        for src in range(SOURCES):
            for k in range(CAP):
                a_parts, b_parts = [], []
                for half in range(2):
                    at = src * ROWS + (2 * k + half) * VALUES
                    index = twice(jnp.broadcast_to(work[at : at + 1, :], (8, 128)))
                    high = jnp.floor(index * (1.0 / LOW))
                    low = index - high * LOW
                    low_all = jnp.concatenate([low] * (LOW // 16), axis=0)
                    b_parts.append(jnp.where(low_all == low_id, one, zero))
                    here = high == high_id
                    wide = [
                        jnp.broadcast_to(work[at + c : at + c + 1, :], (8, 128))
                        for c in range(1, VALUES)
                    ]
                    wide.append(wide[-1])
                    a_parts.append(
                        jnp.concatenate(
                            [
                                jnp.where(
                                    here,
                                    jnp.concatenate(wide[c : c + 2], axis=0).astype(BF16),
                                    zero,
                                )
                                for c in range(0, VALUES, 2)
                            ],
                            axis=0,
                        )
                    )
                a = jnp.concatenate(a_parts, axis=1)
                b = jnp.concatenate(b_parts, axis=1).astype(F8)
                part = lax.dot_general(a, b, NT, preferred_element_type=F32)
                at = pl.multiple_of(heads_smem[k, i * (SOURCES // 2) + src // 2 + src % 2 * (DEVICES // 2)], 8)
                total[pl.ds(at, STRIDE), 0:LOW] += part[0:STRIDE]
        return carry

    lax.fori_loop(0, DEVICES // SOURCES, body, 0)

    for h in range(HIGH):

        def channel(c):
            return total[pl.ds((c - 1) * HIGH + h, BLOCKS, stride=STRIDE), :][:, 0:LOW]

        part = h // (HIGH // 2)
        at = h % (HIGH // 2) * LOW
        divisor = jnp.maximum(channel(1), 1.0)
        tsdf_now[part, :, at : at + LOW] = channel(2) / divisor
        for c in range(3):
            color_now[part, c, :, at : at + LOW] = channel(3 + c) / divisor
        if h % (HIGH // 2) == HIGH // 2 - 1:
            half = pl.ds(part * 256, 256)
            copies += [
                pltpu.make_async_copy(
                    tsdf_now.at[part], tsdf.at[:, half], out_sems.at[1 + 2 * part]
                ),
                pltpu.make_async_copy(
                    color_now.at[part], color.at[:, :, half], out_sems.at[2 + 2 * part]
                ),
            ]
            copies[-2].start()
            copies[-1].start()
    for copy in copies:
        copy.wait()


def pack(sdf_value, weight, color, voxel_index, valid, list_count, list_key, owner_slot):
    given = (
        list_key.reshape(1, LISTS),
        owner_slot.reshape(64, 128),
        list_count.reshape(1, LISTS),
        valid,
        voxel_index,
        weight,
        sdf_value,
        color,
    )
    return pl.pallas_call(
        pack_kernel,
        out_shape=jax.ShapeDtypeStruct((DEVICES * ROWS, 128), BF16),
        in_specs=[pl.BlockSpec(memory_space=pl.ANY)] * 8,
        out_specs=VMEM,
        scratch_shapes=[
            pltpu.VMEM((LISTS, 2 * VALUES * 128), BF16),
            pltpu.VMEM((CAP * DEVICES, LISTS), BF16),
            pltpu.VMEM((SIDE * ROWS, 128), F32),
            pltpu.VMEM((SIDE * ROWS, 128), F32),
            *(pltpu.VMEM(array.shape, array.dtype) for array in given),
            pltpu.SemaphoreType.DMA((8,)),
        ],
        compiler_params=pltpu.CompilerParams(vmem_limit_bytes=20 * 2**20),
        name="pack",
    )(*(pltpu.with_memory_space_constraint(array, pltpu.HBM) for array in given))


def join(got):
    return pl.pallas_call(
        join_kernel,
        out_shape=(
            jax.ShapeDtypeStruct((BLOCKS, 512), F32),
            jax.ShapeDtypeStruct((3, BLOCKS, 512), F32),
            jax.ShapeDtypeStruct((64, 128), I32),
        ),
        in_specs=[VMEM],
        out_specs=[pl.BlockSpec(memory_space=pl.ANY)] * 3,
        scratch_shapes=[
            pltpu.VMEM(((BLOCKS + 1) * STRIDE, 128), F32),
            pltpu.VMEM((SOURCES * ROWS, 128), F32),
            pltpu.VMEM((DEVICES // 2 * GAP, 128), F32),
            pltpu.VMEM((3, TALLY, 128), F32),
            pltpu.VMEM((8, DEVICES), I32),
            pltpu.SMEM((8, DEVICES), I32),
            pltpu.SemaphoreType.DMA,
            pltpu.VMEM((2, BLOCKS, 256), F32),
            pltpu.VMEM((2, 3, BLOCKS, 256), F32),
            pltpu.VMEM((64, 128), I32),
            pltpu.SemaphoreType.DMA((5,)),
        ],
        compiler_params=pltpu.CompilerParams(vmem_limit_bytes=20 * 2**20),
        name="join",
    )(pltpu.with_memory_space_constraint(got, pltpu.VMEM))


def on_device(*given):
    send = pack(*given).reshape(DEVICES, ROWS // 2, 2, 128)
    got = lax.all_to_all(send, AXES, split_axis=0, concat_axis=0, tiled=True)
    tsdf, colors, counts = join(got.reshape(DEVICES * ROWS, 128))
    return tsdf, jnp.transpose(colors, (1, 0, 2)), counts.reshape(DEVICES * BLOCKS)


def solution(mesh):
    return jax.shard_map(
        on_device,
        mesh=mesh,
        in_specs=(
            P(AXES, None),
            P(AXES, None),
            P(None, AXES, None),
            P(AXES, None),
            P(AXES, None),
            P(AXES),
            P(AXES),
            P(),
        ),
        out_specs=(P(AXES, None), P(AXES, None, None), P()),
        check_vma=False,
    )
```

```python
import jax
import jax.numpy as jnp
from jax import lax
from jax.experimental import pallas as pl
from jax.experimental.pallas import tpu as pltpu
from jax.sharding import PartitionSpec as P

AXES = ("view", "tile")
DEVICES = 128
LISTS = 192
PTS = 256
BLOCKS = 64
CAP = 6
VALUES = 6
DATA = CAP * VALUES * 2
ROWS = DATA + 4
PAIR = 2 * ROWS
SIDE = DEVICES // 2
GAP = 20
HIGH = 8
LOW = 64
STRIDE = 40
META = 256
SOURCES = 32
TALLY = DEVICES * LISTS // 128
GROUP = 32
F32 = jnp.float32
BF16 = jnp.bfloat16
I32 = jnp.int32
F8 = jnp.float8_e4m3fn
VMEM = pl.BlockSpec(memory_space=pltpu.VMEM)
NT = (((1,), (1,)), ((), ()))


def iota(shape, dim):
    return lax.broadcasted_iota(I32, shape, dim)


def hot(cond):
    return jnp.where(cond, 1.0, 0.0).astype(BF16)


def dot(a, b):
    return jnp.dot(a, b, preferred_element_type=F32)


def pack_kernel(*refs):
    given, send, x, place, rows = refs[:8], refs[8], refs[9], refs[10], refs[11:13]
    held, sems = refs[13:21], refs[21]
    copies = [
        pltpu.make_async_copy(src, dst, sems.at[i]) for i, (src, dst) in enumerate(zip(given, held))
    ]
    for copy in copies:
        copy.start()
    key, table, count, valid, voxel, weight, sdf, color = held

    copies[0].wait()
    copies[1].wait()
    key_row = key[...]
    high_hot = hot((key_row >> 7) == iota((64, LISTS), 0))
    low_hot = jnp.where((key_row & 127) == iota((128, LISTS), 0), 1.0, 0.0)
    slots = table[...]
    owner_of = (slots >> 6).astype(F32).T.astype(BF16)
    row_of = (slots & 63).astype(F32).T.astype(BF16)
    owner = jnp.sum(dot(owner_of, high_hot) * low_hot, axis=0, keepdims=True)
    row = jnp.sum(dot(row_of, high_hot) * low_hot, axis=0, keepdims=True)
    owner_hot = jnp.where(owner.astype(I32) == iota((DEVICES, LISTS), 0), 1.0, 0.0)
    before = hot(iota((LISTS, LISTS), 0) < iota((LISTS, LISTS), 1))
    order = jnp.sum(dot(owner_hot.astype(BF16), before) * owner_hot, axis=0, keepdims=True)
    for side in range(2):
        for k in range(CAP):
            at = (side * CAP + k) * SIDE
            place[at : at + SIDE, :] = jnp.where(
                order == k, owner_hot[side * SIDE : (side + 1) * SIDE], 0.0
            ).astype(BF16)

    copies[2].wait()
    copies[3].wait()
    diagonal = iota((LISTS, LISTS), 0) == iota((LISTS, LISTS), 1)
    spread = jnp.where(diagonal, count[...].astype(F32), 0.0).astype(BF16)
    used = dot(spread, jnp.ones((LISTS, PTS), BF16))
    live = (iota((LISTS, PTS), 1).astype(F32) < used) & (valid[...] == 1)
    mask = jnp.where(live, 1.0, 0.0)
    live_count = lax.dot_general(
        jnp.ones((8, PTS), BF16), mask.astype(BF16), NT, preferred_element_type=F32
    )[0:1]
    storage = owner * BLOCKS + row
    high = jnp.floor(storage * (1.0 / 128))
    code = storage - high * 128.0 + 128.0
    high_bits = high.astype(I32)
    for bit in range(6):
        code = jnp.where((high_bits >> bit) & 1 == 1, code * 2.0 ** (1 << bit), code)
    odd = (lax.axis_index("tile") & 1) == 1
    blank = jnp.zeros((1, 64), F32)
    lines = []
    for line in (code, live_count):
        rest = line[:, 128:LISTS]
        lines += [
            line[:, 0:128],
            jnp.where(
                odd,
                jnp.concatenate([blank, rest], axis=1),
                jnp.concatenate([rest, blank], axis=1),
            ),
        ]
    head = jnp.concatenate(lines, axis=0)

    for i in range(SIDE):
        for side in range(2):
            rows[side][i * ROWS + DATA : (i + 1) * ROWS, :] = head

    for copy in copies[4:]:
        copy.wait()
    scaled = mask * weight[...]
    values = [
        (voxel[...] - 256).astype(F32),
        scaled,
        scaled * sdf[...],
        scaled * color[0],
        scaled * color[1],
        scaled * color[2],
    ]
    for v, value in enumerate(values):
        value = value.astype(BF16)
        for half in range(2):
            j = half * VALUES + v
            x[:, j * 128 : (j + 1) * 128] = value[:, half * 128 : (half + 1) * 128]

    def move(side, j):
        span = slice(side * CAP * SIDE, (side + 1) * CAP * SIDE)
        moved = dot(place[span, :], x[:, j * 128 : (j + 2) * 128])
        for k in range(CAP):
            for part in range(2):
                at = k * 2 * VALUES + j + part
                rows[side][pl.ds(at, SIDE, stride=ROWS), :] = moved[
                    k * SIDE : (k + 1) * SIDE, part * 128 : (part + 1) * 128
                ]

    def convert(side, pair):
        at = pair * PAIR
        to = side * SIDE * ROWS + at
        send[to : to + PAIR, :] = rows[side][at : at + PAIR, :].astype(BF16)

    for j in range(0, 2 * VALUES, 2):
        move(0, j)
    for j in range(0, 2 * VALUES, 2):
        move(1, j)
        for pair in range(j * SIDE // 24, (j + 2) * SIDE // 24):
            convert(0, pair)
    for pair in range(SIDE // 2):
        convert(1, pair)


def twice(rows8):
    return jnp.concatenate([rows8, rows8], axis=0).astype(BF16)


def ids(count):
    return [(iota((16, 128), 0) + 16 * j).astype(F32).astype(BF16) for j in range(count)]


def join_kernel(got, tsdf, color, counts, total, work, info, lines, heads, heads_smem, sem):
    me = lax.axis_index("view") * 16 + lax.axis_index("tile")
    one, zero = jnp.ones((), BF16), jnp.zeros((), BF16)

    def unpack_head(i, carry):
        for side in range(2):
            at = pl.multiple_of(i * PAIR + DATA * (side + 1), 8)
            info[pl.ds(i * GAP + 8 * side, 8), :] = got[pl.ds(at, 8), :].astype(F32)
        return carry

    lax.fori_loop(0, DEVICES // 2, unpack_head, 0, unroll=16)

    def line(p):
        return jnp.concatenate(
            [info[pl.ds(p + 12 * side, DEVICES // 2, stride=GAP), :] for side in range(2)], axis=0
        )

    def decoded(code):
        high = jnp.zeros_like(code)
        for bit in range(5, -1, -1):
            step = float(1 << bit)
            over = code >= 128.0 * 2.0**step
            code = jnp.where(over, code * 2.0**-step, code)
            high = jnp.where(over, high + step, high)
        return high, code - 128.0

    full = (*decoded(line(0)), line(2))
    rest = (*decoded(line(1)), line(3))
    row = jnp.concatenate([full[0] * 128.0 + full[1], rest[0] * 128.0 + rest[1]], axis=1)
    row = row - (me * BLOCKS).astype(F32)
    mine = (row >= 0.0) & (row < float(BLOCKS))
    before = hot(iota((META, META), 0) < iota((META, META), 1))
    order = dot(hot(mine), before)
    found = jnp.zeros((8, DEVICES), F32)
    for k in range(CAP):
        picked = jnp.where((order == k) & mine, row + 1.0, 0.0).astype(BF16)
        select = hot(iota((8, META), 0) == k)
        found += lax.dot_general(select, picked, NT, preferred_element_type=F32)
    found = found.astype(I32)
    heads[...] = jnp.where(found == 0, BLOCKS, found - 1) * STRIDE
    copy = pltpu.make_async_copy(heads, heads_smem, sem)
    total[...] = jnp.zeros_like(total)

    left = iota((DEVICES // 2, 128), 1) < 64
    for p in range(3):
        lines[p, 0:DEVICES, :] = full[p]
        lines[p, DEVICES:TALLY, :] = jnp.where(
            left, rest[p][0 : DEVICES // 2], rest[p][DEVICES // 2 : DEVICES]
        )
    copy.start()
    tally_ids = ids(8)

    def tally(g, sums):
        a_parts, b_parts = [], []
        for t in range(GROUP):
            high, low, number = [
                twice(jnp.broadcast_to(lines[p, pl.ds(g * GROUP + t, 1), :], (8, 128)))
                for p in range(3)
            ]
            a_parts.append(
                jnp.concatenate([jnp.where(high == tally_ids[j], number, zero) for j in range(4)], 0)
            )
            b_parts.append(
                jnp.concatenate([jnp.where(low == tally_ids[j], one, zero) for j in range(8)], 0)
            )
        a = jnp.concatenate(a_parts, axis=1)
        b = jnp.concatenate(b_parts, axis=1).astype(F8)
        return sums + lax.dot_general(a, b, NT, preferred_element_type=F32)

    sums = lax.fori_loop(0, TALLY // GROUP, tally, jnp.zeros((64, 128), F32))
    counts[...] = sums.astype(I32)
    copy.wait()

    low_id = iota((LOW, 128), 0).astype(F32).astype(BF16)
    high_id = ((iota((16, 128), 0) & 7) - 4).astype(F32).astype(BF16)

    def body(i, carry):
        for pair in range(SOURCES // 2):
            at = pl.multiple_of((i * (SOURCES // 2) + pair) * PAIR, 8)
            work[pair * PAIR : (pair + 1) * PAIR, :] = got[pl.ds(at, PAIR), :].astype(F32)
        for src in range(SOURCES):
            for k in range(CAP):
                a_parts, b_parts = [], []
                for half in range(2):
                    at = src * ROWS + (2 * k + half) * VALUES
                    index = twice(jnp.broadcast_to(work[at : at + 1, :], (8, 128)))
                    high = jnp.floor(index * (1.0 / LOW))
                    low = index - high * LOW
                    low_all = jnp.concatenate([low] * (LOW // 16), axis=0)
                    b_parts.append(jnp.where(low_all == low_id, one, zero))
                    here = high == high_id
                    wide = [
                        jnp.broadcast_to(work[at + c : at + c + 1, :], (8, 128))
                        for c in range(1, VALUES)
                    ]
                    wide.append(wide[-1])
                    a_parts.append(
                        jnp.concatenate(
                            [
                                jnp.where(
                                    here,
                                    jnp.concatenate(wide[c : c + 2], axis=0).astype(BF16),
                                    zero,
                                )
                                for c in range(0, VALUES, 2)
                            ],
                            axis=0,
                        )
                    )
                a = jnp.concatenate(a_parts, axis=1)
                b = jnp.concatenate(b_parts, axis=1).astype(F8)
                part = lax.dot_general(a, b, NT, preferred_element_type=F32)
                at = pl.multiple_of(heads_smem[k, i * (SOURCES // 2) + src // 2 + src % 2 * (DEVICES // 2)], 8)
                total[pl.ds(at, STRIDE), 0:LOW] += part[0:STRIDE]
        return carry

    lax.fori_loop(0, DEVICES // SOURCES, body, 0)

    for h in range(HIGH):

        def channel(c):
            return total[pl.ds((c - 1) * HIGH + h, BLOCKS, stride=STRIDE), :][:, 0:LOW]

        span = slice(h * LOW, (h + 1) * LOW)
        divisor = jnp.maximum(channel(1), 1.0)
        tsdf[:, span] = channel(2) / divisor
        for c in range(3):
            color[c, :, span] = channel(3 + c) / divisor


def pack(sdf_value, weight, color, voxel_index, valid, list_count, list_key, owner_slot):
    given = (
        list_key.reshape(1, LISTS),
        owner_slot.reshape(64, 128),
        list_count.reshape(1, LISTS),
        valid,
        voxel_index,
        weight,
        sdf_value,
        color,
    )
    return pl.pallas_call(
        pack_kernel,
        out_shape=jax.ShapeDtypeStruct((DEVICES * ROWS, 128), BF16),
        in_specs=[pl.BlockSpec(memory_space=pl.ANY)] * 8,
        out_specs=VMEM,
        scratch_shapes=[
            pltpu.VMEM((LISTS, 2 * VALUES * 128), BF16),
            pltpu.VMEM((CAP * DEVICES, LISTS), BF16),
            pltpu.VMEM((SIDE * ROWS, 128), F32),
            pltpu.VMEM((SIDE * ROWS, 128), F32),
            *(pltpu.VMEM(array.shape, array.dtype) for array in given),
            pltpu.SemaphoreType.DMA((8,)),
        ],
        compiler_params=pltpu.CompilerParams(vmem_limit_bytes=20 * 2**20),
        name="pack",
    )(*(pltpu.with_memory_space_constraint(array, pltpu.HBM) for array in given))


def join(got):
    return pl.pallas_call(
        join_kernel,
        out_shape=(
            jax.ShapeDtypeStruct((BLOCKS, 512), F32),
            jax.ShapeDtypeStruct((3, BLOCKS, 512), F32),
            jax.ShapeDtypeStruct((64, 128), I32),
        ),
        in_specs=[VMEM],
        out_specs=(VMEM, VMEM, VMEM),
        scratch_shapes=[
            pltpu.VMEM(((BLOCKS + 1) * STRIDE, 128), F32),
            pltpu.VMEM((SOURCES * ROWS, 128), F32),
            pltpu.VMEM((DEVICES // 2 * GAP, 128), F32),
            pltpu.VMEM((3, TALLY, 128), F32),
            pltpu.VMEM((8, DEVICES), I32),
            pltpu.SMEM((8, DEVICES), I32),
            pltpu.SemaphoreType.DMA,
        ],
        compiler_params=pltpu.CompilerParams(vmem_limit_bytes=20 * 2**20),
        name="join",
    )(pltpu.with_memory_space_constraint(got, pltpu.VMEM))


def on_device(*given):
    send = pack(*given).reshape(DEVICES, ROWS // 2, 2, 128)
    got = lax.all_to_all(send, AXES, split_axis=0, concat_axis=0, tiled=True)
    tsdf, colors, counts = join(got.reshape(DEVICES * ROWS, 128))
    return tsdf, jnp.transpose(colors, (1, 0, 2)), counts.reshape(DEVICES * BLOCKS)


def solution(mesh):
    return jax.shard_map(
        on_device,
        mesh=mesh,
        in_specs=(
            P(AXES, None),
            P(AXES, None),
            P(None, AXES, None),
            P(AXES, None),
            P(AXES, None),
            P(AXES),
            P(AXES),
            P(),
        ),
        out_specs=(P(AXES, None), P(AXES, None, None), P()),
        check_vma=False,
    )
```
